512 devices in a mesh: row: 16 (over z, core), col: 32 (over y, x).
Axes of the slice: x: 4, y: 8, z: 8, core: 2. Of those that a mesh axis runs over, the one named last changes fastest.
Arguments:
- ainv: float32 [4, 2048, 2, 4096], P(None, 'row', None, 'col'), may hold values from -6 to 6
- lhat_first: float32 [4, 2048, 512], P(None, ('row', 'col')), may hold values from -0.078125 to 0.078125
- lhat_second: float32 [4, 2048, 512], P(None, ('row', 'col')), may hold values from -0.09375 to 0.09375
- second_on_first: float32 [512, 512], replicated, may hold values from -0.25 to 0.25
- dinv_first: float32 [512, 512], P(None, 'col'), may hold values from -6 to 6
- dinv_second: float32 [512, 512], P(None, 'col'), may hold values from -6 to 6
- anc_first: int32 [48], replicated, may hold values from 0 to 63, as said below
- anc_second: int32 [32], replicated, may hold values from 0 to 63, as said below
Outputs:
- cross_first: float32 [4, 2048, 512], P(None, 'row', 'col')
- diag_first: float32 [512, 512], P(None, 'col')
- cross_second: float32 [4, 2048, 512], P(None, 'row', 'col')
- link_second: float32 [512, 512], P(None, 'col')
- diag_second: float32 [512, 512], P(None, 'col')
The draws below stay inside these ranges and needn't reach their ends.
Inputs may be any that keep to these rules, and one draw needn't show every extreme that they name: `anc_first`: 48 different tile numbers in increasing order. `anc_second`: 32 different tile numbers in increasing order, each also listed in anc_first.
All inputs are finite; a program needn't handle non-finite values.
Results may differ from the reference program's by a relative error of at most 0.000088.
Values sent between devices are 32-bit elements; how exact they have to be, the bound alone decides.
A program may use at most 64 MiB of HBM per device.

```python
import jax
import jax.numpy as jnp
from jax import lax

KW = 512
TILE = 128
STRIPS = 2
NT = 64
NL1 = 48
NL2 = 32
N_ROW = 16
N_COL = 32


def ancestor_sets(key):
    order = jax.random.permutation(jax.random.fold_in(key, 7), NT)
    first = jnp.sort(order[:NL1]).astype(jnp.int32)
    pick = jax.random.permutation(jax.random.fold_in(key, 11), NL1)
    second = jnp.sort(first[pick[:NL2]]).astype(jnp.int32)
    return (first, second)


def draw_anc_first(key, part):
    return ancestor_sets(key)[0]


def draw_anc_second(key, part):
    return ancestor_sets(key)[1]


def shard_levels(key, dims, shards, smallest, top_value):
    def one(axis_at, shards_of):
        steps = jax.random.uniform(jax.random.fold_in(jax.random.fold_in(key, 6), axis_at), (shards_of,), jnp.float32, smallest / len(shards), top_value / len(shards))
        return jnp.repeat(jnp.exp(steps), dims[axis_at] // shards_of).reshape((-1,) + (1,) * (len(dims) - axis_at - 1))

    factor_of = one(*shards[0])
    for cut in shards[1:]:
        factor_of = factor_of * one(*cut)
    return factor_of


def centred(rng, dims, scale, limit, cuts=(), kind=jnp.bfloat16):
    result = jax.random.normal(rng, dims, jnp.float32) * scale
    if len(cuts) > 0:
        result = shard_levels(rng, dims, cuts, -0.22, 0.18) * result
    return jnp.clip(result, min=-limit, max=limit).astype(kind)


def setup_inputs(seed: int = 0) -> dict:
    keys = jax.random.split(jax.random.key(seed), 9)
    ainv = centred(keys[0], (NT // N_ROW, N_ROW * TILE, STRIPS, N_COL * TILE), 1.0, 6.0, ((1, 16), (3, 32)), jnp.float32)
    lhat_first = centred(keys[1], (NT // N_ROW, N_ROW * TILE, KW), (NL1 * TILE) ** -0.5, 0.078125, ((1, 512),), jnp.float32)
    lhat_second = centred(keys[2], (NT // N_ROW, N_ROW * TILE, KW), (NL2 * TILE) ** -0.5, 0.09375, ((1, 512),), jnp.float32)
    second_on_first = centred(keys[3], (KW, KW), KW ** -0.5, 0.25, (), jnp.float32)
    dinv_first = centred(keys[4], (KW, KW), 1.0, 6.0, ((1, 32),), jnp.float32)
    dinv_second = centred(keys[5], (KW, KW), 1.0, 6.0, ((1, 32),), jnp.float32)
    anc_first = draw_anc_first(jax.random.fold_in(keys[8], 71), 0)
    anc_second = draw_anc_second(jax.random.fold_in(keys[8], 71), 0)
    return {"ainv": ainv, "lhat_first": lhat_first, "lhat_second": lhat_second, "second_on_first": second_on_first, "dinv_first": dinv_first, "dinv_second": dinv_second, "anc_first": anc_first, "anc_second": anc_second}


def product(left, right):
    return jnp.dot(left, right, precision=lax.Precision.HIGHEST, preferred_element_type=jnp.float32)


def reference(ainv, lhat_first, lhat_second, second_on_first, dinv_first, dinv_second, anc_first, anc_second):
    inverse = ainv.reshape(NT * TILE, NT * TILE)
    tiles = jnp.arange(NT, dtype=jnp.int32)

    def row_keep(listing):
        listed = jnp.any(tiles[:, None] == listing[None, :].astype(jnp.int32), axis=1)
        return jnp.repeat(listed.astype(jnp.float32), TILE)[:, None]

    keep_first = row_keep(anc_first)
    keep_second = row_keep(anc_second)
    left_first = lhat_first.reshape(NT * TILE, KW) * keep_first
    left_second = lhat_second.reshape(NT * TILE, KW) * keep_second
    cross_first = -keep_first * product(inverse, left_first)
    diag_first = dinv_first - product(left_first.T, cross_first)
    cross_second = -keep_second * (product(inverse, left_second) + product(cross_first, second_on_first))
    link_second = -(product(cross_first.T, left_second) + product(diag_first.T, second_on_first))
    diag_second = dinv_second - (product(left_second.T, cross_second) + product(second_on_first.T, link_second))
    shape_out = (NT // N_ROW, N_ROW * TILE, KW)
    return cross_first.reshape(shape_out), diag_first, cross_second.reshape(shape_out), link_second, diag_second
```

```python
import functools

import jax
import jax.numpy as jnp
from jax import lax
from jax.experimental import pallas as pl
from jax.experimental.pallas import tpu as pltpu
from jax.sharding import PartitionSpec as P

MESH = pl.DeviceIdType.MESH
F32 = jnp.float32
BF16 = jnp.bfloat16
X, Y, Z = 4, 8, 8
NR, NC = 16, 32


def split(value):
    high = value.astype(BF16)
    return high, (value - high.astype(F32)).astype(BF16)


def mm(left, right):
    return jnp.dot(left, right, preferred_element_type=F32)


def mm3(left, right_high, right_low):
    high, low = split(left)
    return mm(high, right_high) + (mm(low, right_high) + mm(high, right_low))


def kernel(
    a_hbm, s_hbm, l1_ref, l2_ref, d1_ref, d2_ref, anc1_ref, anc2_ref,
    cross1_ref, diag1_ref, cross2_ref, link_ref, diag2_ref,
    abuf, sbuf, s_high, s_low, rbuf, own, mbuf, m_high, m_low, pt, cr,
    tt, ts, tr, ls, lr, r0, tg, tsum, gb, lsum, xt, lk,
    local_sem, a_send, a_recv, my_send, my_recv, mx_send, mx_recv, sc_send, sc_recv,
    ag_send, ag_recv, dd_send, dd_recv, rs_send, rs_recv, t_send, t_recv, l_send, l_recv,
    tg_send, tg_recv, g_send, g_recv, b_send, b_recv,
):
    r, c = lax.axis_index("row"), lax.axis_index("col")
    z, core = r // 2, r % 2
    y, x = c // X, c % X
    right, left = (x + 1) % X, (x + X - 1) % X
    across = (x + 2) % X

    def remote(src, dst, send, recv, row, col):
        return pltpu.make_async_remote_copy(
            src_ref=src, dst_ref=dst, send_sem=send, recv_sem=recv,
            device_id=(row, col), device_id_type=MESH,
        )

    sent = []

    def start(copy):
        copy.start()
        sent.append(copy)

    a_copy = pltpu.make_async_copy(a_hbm, abuf.at[x], local_sem.at[0])
    a_copy.start()
    s_copy = pltpu.make_async_copy(s_hbm, sbuf, local_sem.at[1])
    s_copy.start()

    tile_ids = lax.broadcasted_iota(jnp.int32, (4, 1), 0) * NR + r

    def keeps(anc_ref):
        hits = jnp.where(anc_ref[...] == tile_ids, 1.0, 0.0).astype(F32)
        return jnp.max(hits, axis=1, keepdims=True)

    keep1, keep2 = keeps(anc1_ref), keeps(anc2_ref)
    rows1 = [l1_ref[a] * keep1[a : a + 1] for a in range(4)]
    rows2 = [l2_ref[a] * keep2[a : a + 1] for a in range(4)]

    def a_part(slot, half):
        return abuf.at[slot, pl.ds(half * 512, 512)]

    def a_move(slot, half, send, to):
        part = a_part(slot, half)
        return remote(part, part, a_send.at[send], a_recv.at[slot, half], r, y * X + to)

    a_copy.wait()
    start(a_move(x, 0, 0, right))
    start(a_move(x, 1, 1, left))
    start(a_move(x, 1, 2, right))
    start(a_move(x, 0, 3, left))

    s_copy.wait()
    sh, sl = split(sbuf[...])
    s_high[...] = sh
    s_low[...] = sl
    m1 = jnp.concatenate(rows1, axis=0)
    n2 = jnp.concatenate(rows2, axis=0) - mm3(m1, s_high[...], s_low[...])
    for a in range(4):
        yh, s = a % 2, a // 2
        for k in range(4):
            lanes = slice(k * 128, (k + 1) * 128)
            own[yh, k, s, pl.ds(0, 4, stride=2), :] = rows1[a][:, lanes]
            own[yh, k, s, pl.ds(1, 4, stride=2), :] = n2[a * 4 : a * 4 + 4, lanes]
    xs = r % X
    for yh in range(2):
        for k in range(4):
            to_col = (r // X + 4 * yh) * X + k
            here = jnp.logical_and(c // 2 == r, c == to_col)
            copy = remote(
                own.at[yh, k], mbuf.at[xs, :, c], sc_send.at[yh, k], sc_recv.at[xs, c % 2],
                c // 2, to_col,
            )

            @pl.when(jnp.logical_not(here))
            def _():
                copy.start()

            @pl.when(here)
            def _():
                mbuf[xs, :, c] = own[yh, k]

    rflat = rbuf
    for a in range(4):
        for k in range(4):
            lanes = slice(k * 128, (k + 1) * 128)
            rflat[a, y, x, pl.ds(k, 4, stride=8), :] = rows1[a][:, lanes]
            rflat[a, y, x, pl.ds(4 + k, 4, stride=8), :] = rows2[a][:, lanes]

    for xq in range(4):
        for par in range(2):
            from_row = (y % 4) * X + xq
            from_col = 2 * r + par
            here = jnp.logical_and(from_row == r, from_col == c)
            copy = remote(
                own.at[0, 0], mbuf.at[xq, :, from_col], sc_send.at[0, 0], sc_recv.at[xq, par],
                from_row, from_col,
            )

            @pl.when(jnp.logical_not(here))
            def _():
                copy.wait_recv()

    def slab(row):
        return mbuf.at[:, :, pl.ds(2 * row, 2)]

    for d in (1, 7, 2, 6, 3, 5, 4):
        to = (z + d) % Z
        start(remote(slab(r), slab(r), ag_send.at[d], ag_recv.at[z], to * 2 + core, c))
    start(remote(slab(r), slab(r), dd_send.at[z], dd_recv.at[z], z * 2 + 1 - core, c))

    def r_part(yy, xx):
        return rbuf.at[:, yy, xx]

    for d in (1, 7, 2, 6, 3, 5, 4):
        to = (y + d) % Y
        start(remote(r_part(y, x), r_part(y, x), my_send.at[d], my_recv.at[y], r, to * X + x))

    def a_wait(slot, half):
        a_move(slot, half, 0, right).wait_recv()

    a_wait(left, 0)
    start(a_move(left, 0, 4, right))
    a_wait(right, 1)
    start(a_move(right, 1, 5, left))

    for d in (7, 1, 6, 2, 5, 3, 4):
        zs = (z + d) % Z
        part = slab(zs * 2 + core)
        remote(part, part, ag_send.at[d], ag_recv.at[zs], r, c).wait_recv()
        start(remote(part, part, dd_send.at[zs], dd_recv.at[zs], z * 2 + 1 - core, c))

    d1 = d1_ref[...]
    r0_full = mm3(d1, s_high[...], s_low[...])
    for k in range(4):
        r0[k] = r0_full[:, k * 128 : (k + 1) * 128]

    for d in (7, 1, 6, 2, 5, 3, 4):
        ys = (y + d) % Y
        part = r_part(ys, x)
        remote(part, part, my_send.at[d], my_recv.at[ys], r, c).wait_recv()

    def r_move(slot, half, send, to):
        part = rbuf.at[pl.ds(half * 2, 2), :, slot]
        return remote(part, part, mx_send.at[send], mx_recv.at[slot, half], r, y * X + to)

    start(r_move(x, 0, 0, right))
    start(r_move(x, 1, 1, left))
    start(r_move(x, 1, 2, right))
    start(r_move(x, 0, 3, left))

    for zs in range(Z):
        part = slab(zs * 2 + 1 - core)
        remote(part, part, dd_send.at[zs], dd_recv.at[zs], r, c).wait_recv()
    a_wait(left, 1)
    a_wait(right, 0)
    a_wait(across, 0)
    a_wait(across, 1)

    def split_columns(step, carry):
        xq, s = step // 2, step % 2
        flat = mbuf.at[xq, s].reshape(256, 128)
        for m in range(2):
            high, low = split(flat[pl.ds(m, 128, stride=2), :])
            at = pl.ds(pl.multiple_of(s * 128, 128), 128)
            m_high[xq, at, m * 128 : (m + 1) * 128] = high
            m_low[xq, at, m * 128 : (m + 1) * 128] = low
        return carry

    lax.fori_loop(0, 8, split_columns, 0)

    def multiply(rb, carry):
        acc = jnp.zeros((128, 256), F32)
        for xq in range(4):
            both = [abuf[xq, pl.ds(rb * 256 + s, 128, stride=2), :] for s in range(2)]
            acc = acc + mm3(jnp.concatenate(both, axis=1), m_high[xq], m_low[xq])
        for m in range(2):
            pt[rb, m] = acc[:, m * 128 : (m + 1) * 128].T
        return carry

    lax.fori_loop(0, 4, multiply, 0)

    for blk in range(8):
        to_y = 2 * x + blk // X
        to_col = to_y * X + blk % X
        src = pt.at[:, :, pl.ds(blk * 16, 16)]
        here = to_col == c
        copy = remote(src, cr.at[y], rs_send.at[blk], rs_recv.at[y], r, to_col)

        @pl.when(jnp.logical_not(here))
        def _():
            copy.start()

        @pl.when(here)
        def _():
            cr[y] = pt[:, :, pl.ds(blk * 16, 16)]

    def r_wait(slot, half):
        r_move(slot, half, 0, right).wait_recv()

    r_wait(left, 0)
    start(r_move(left, 0, 4, right))
    r_wait(right, 1)
    start(r_move(right, 1, 5, left))

    from_x = y // 2
    for ys in range(8):
        here = jnp.logical_and(ys == y, from_x == x)
        copy = remote(
            pt.at[:, :, pl.ds(0, 16)], cr.at[ys], rs_send.at[0], rs_recv.at[ys],
            r, ys * X + from_x,
        )

        @pl.when(jnp.logical_not(here))
        def _():
            copy.wait_recv()

    first, second = [], []
    for a in range(4):
        sum1, sum2 = cr[0, a, 0], cr[0, a, 1]
        for ys in range(1, 8):
            sum1 = sum1 + cr[ys, a, 0]
            sum2 = sum2 + cr[ys, a, 1]
        sum1 = -keep1[a : a + 1] * sum1
        sum2 = -keep2[a : a + 1] * sum2
        cross1_ref[a] = sum1
        cross2_ref[a] = sum2
        first.append(sum1)
        second.append(sum2)
    both = jnp.concatenate(
        [jnp.concatenate(first, axis=1), jnp.concatenate(second, axis=1)], axis=0
    )
    c_high, c_low = split(both)

    r_wait(left, 1)
    r_wait(right, 0)
    r_wait(across, 0)
    r_wait(across, 1)

    rows_all = rbuf.reshape(4096, 128)
    for q in range(8):
        high, low = split(rows_all[pl.ds(q, 512, stride=8), :])
        tt[q] = mm(c_high, high) + (mm(c_low, high) + mm(c_high, low))

    q1 = jnp.concatenate([tt[k, 0:16] for k in range(4)], axis=1)
    rows = mm3(q1, s_high[...], s_low[...])
    for k in range(4):
        ls[k] = rows[:, k * 128 : (k + 1) * 128] - tt[4 + k, 0:16]
        for half in range(2):
            ts[k * 2 + half] = tt[k, half * 8 : half * 8 + 8]
            ts[8 + k * 2 + half] = tt[4 + k, 16 + half * 8 : 24 + half * 8]

    def send_link(q, carry):
        copy = remote(ls.at[q], lr.at[r], l_send.at[q], l_recv.at[r], 4 * q, c)

        @pl.when(r != 4 * q)
        def _():
            copy.start()

        return carry

    lax.fori_loop(0, 4, send_link, 0)

    def send_sum(d, carry):
        to = (r + d) % NR
        remote(ts.at[to], tr.at[r], t_send.at[d], t_recv.at[r], to, c).start()
        return carry

    lax.fori_loop(1, NR, send_sum, 0)
    tr[r] = ts[r]
    q_own = r // 4
    collects = r % 4 == 0

    @pl.when(collects)
    def _():
        lr[r] = ls[q_own]

        def take(d, carry):
            src = (r + d) % NR
            remote(ls.at[0], lr.at[src], l_send.at[0], l_recv.at[src], src, c).wait_recv()
            return carry

        lax.fori_loop(1, NR, take, 0)
        total = lr[0]
        for src in range(1, NR):
            total = total + lr[src]
        lsum[...] = total - r0[q_own]
        for j in range(8):
            to_col = 8 * q_own + j
            copy = remote(lsum, gb.at[c], g_send.at[j], g_recv.at[c], r, to_col)

            @pl.when(to_col != c)
            def _():
                copy.start()

    def take_sum(d, carry):
        src = (r + d) % NR
        remote(ts.at[0], tr.at[src], t_send.at[0], t_recv.at[src], src, c).wait_recv()
        return carry

    lax.fori_loop(1, NR, take_sum, 0)
    total = tr[0]
    for src in range(1, NR):
        total = total + tr[src]
    tsum[...] = total
    tg[r] = total

    def send_total(d, carry):
        to = (r + d) % NR
        remote(tsum, tg.at[r], tg_send.at[d], tg_recv.at[r], to, c).start()
        return carry

    lax.fori_loop(1, NR, send_total, 0)

    root_row = 4 * (c // 8)
    is_root = r == root_row

    @pl.when(is_root)
    def _():
        gb[c] = lsum[...]

        def take(d, carry):
            src = (c + d) % NC
            remote(lsum, gb.at[src], g_send.at[0], g_recv.at[src], r, src).wait_recv()
            return carry

        lax.fori_loop(1, NC, take, 0)
        for k in range(4):
            block = gb[8 * k : 8 * k + 8].reshape(128, 128)
            xt[k] = block.T
        for k in range(4):
            lk[:, k * 128 : (k + 1) * 128] = xt[k, pl.ds(pl.multiple_of(16 * (c % 8), 16), 16), :]

        def send_on(d, carry):
            to = (r + d) % NR
            remote(lk, lk, b_send.at[d], b_recv, to, c).start()
            return carry

        lax.fori_loop(1, NR, send_on, 0)

    def take_total(d, carry):
        src = (r + d) % NR
        remote(tsum, tg.at[src], tg_send.at[0], tg_recv.at[src], src, c).wait_recv()
        return carry

    lax.fori_loop(1, NR, take_total, 0)
    for k in range(4):
        lanes = slice(k * 128, (k + 1) * 128)
        sum1 = jnp.concatenate([tg[2 * k], tg[2 * k + 1]], axis=0)
        diag1_ref[:, lanes] = d1_ref[:, lanes] - sum1

    @pl.when(jnp.logical_not(is_root))
    def _():
        remote(lk, lk, b_send.at[0], b_recv, root_row, c).wait_recv()

    link = lk[...]
    link_ref[...] = link
    tail = mm3(link, s_high[...], s_low[...])
    for k in range(4):
        lanes = slice(k * 128, (k + 1) * 128)
        sum2 = jnp.concatenate([tg[8 + 2 * k], tg[9 + 2 * k]], axis=0)
        diag2_ref[:, lanes] = d2_ref[:, lanes] - (sum2 + tail[:, lanes])

    for copy in sent:
        copy.wait_send()
    for yh in range(2):
        for k in range(4):
            to_col = (r // X + 4 * yh) * X + k
            here = jnp.logical_and(c // 2 == r, c == to_col)

            @pl.when(jnp.logical_not(here))
            def _():
                remote(
                    own.at[yh, k], mbuf.at[xs, :, c], sc_send.at[yh, k], sc_recv.at[xs, c % 2],
                    c // 2, to_col,
                ).wait_send()

    for blk in range(8):
        to_col = (2 * x + blk // X) * X + blk % X

        @pl.when(to_col != c)
        def _():
            remote(
                pt.at[:, :, pl.ds(blk * 16, 16)], cr.at[y], rs_send.at[blk], rs_recv.at[y],
                r, to_col,
            ).wait_send()

    def link_left(q, carry):
        @pl.when(r != 4 * q)
        def _():
            remote(ls.at[q], lr.at[r], l_send.at[q], l_recv.at[r], 4 * q, c).wait_send()

        return carry

    lax.fori_loop(0, 4, link_left, 0)

    def sums_left(d, carry):
        to = (r + d) % NR
        remote(ts.at[to], tr.at[r], t_send.at[d], t_recv.at[r], to, c).wait_send()
        remote(tsum, tg.at[r], tg_send.at[d], tg_recv.at[r], to, c).wait_send()
        return carry

    lax.fori_loop(1, NR, sums_left, 0)

    @pl.when(collects)
    def _():
        for j in range(8):
            to_col = 8 * q_own + j

            @pl.when(to_col != c)
            def _():
                remote(lsum, gb.at[c], g_send.at[j], g_recv.at[c], r, to_col).wait_send()

    @pl.when(is_root)
    def _():
        def on_left(d, carry):
            remote(lk, lk, b_send.at[d], b_recv, (r + d) % NR, c).wait_send()
            return carry

        lax.fori_loop(1, NR, on_left, 0)


def body(
    ainv, lhat_first, lhat_second, second_on_first, dinv_first, dinv_second, anc_first, anc_second
):
    vmem = pl.BlockSpec(memory_space=pltpu.VMEM)
    hbm = pl.BlockSpec(memory_space=pl.ANY)
    dma = pltpu.SemaphoreType.DMA
    cross = jax.ShapeDtypeStruct((4, 16, 128), F32)
    panel = jax.ShapeDtypeStruct((16, 512), F32)
    cross1, diag1, cross2, link, diag2 = pl.pallas_call(
        kernel,
        out_shape=(cross, panel, cross, panel, panel),
        in_specs=[hbm, hbm] + [vmem] * 6,
        out_specs=(vmem,) * 5,
        scratch_shapes=[
            pltpu.VMEM((4, 1024, 128), F32),
            pltpu.VMEM((512, 512), F32),
            pltpu.VMEM((512, 512), BF16),
            pltpu.VMEM((512, 512), BF16),
            pltpu.VMEM((4, 8, 4, 32, 128), F32),
            pltpu.VMEM((2, 4, 2, 8, 128), F32),
            pltpu.VMEM((4, 2, 32, 8, 128), F32),
            pltpu.VMEM((4, 256, 256), BF16),
            pltpu.VMEM((4, 256, 256), BF16),
            pltpu.VMEM((4, 2, 128, 128), F32),
            pltpu.VMEM((8, 4, 2, 16, 128), F32),
            pltpu.VMEM((8, 32, 128), F32),
            pltpu.VMEM((16, 8, 128), F32),
            pltpu.VMEM((16, 8, 128), F32),
            pltpu.VMEM((4, 16, 128), F32),
            pltpu.VMEM((16, 16, 128), F32),
            pltpu.VMEM((4, 16, 128), F32),
            pltpu.VMEM((16, 8, 128), F32),
            pltpu.VMEM((8, 128), F32),
            pltpu.VMEM((32, 16, 128), F32),
            pltpu.VMEM((16, 128), F32),
            pltpu.VMEM((4, 128, 128), F32),
            pltpu.VMEM((16, 512), F32),
            dma((2,)),
            dma((6,)), dma((4, 2)),
            dma((8,)), dma((8,)),
            dma((6,)), dma((4, 2)),
            dma((2, 4)), dma((4, 2)),
            dma((8,)), dma((8,)),
            dma((8,)), dma((8,)),
            dma((8,)), dma((8,)),
            dma((16,)), dma((16,)),
            dma((4,)), dma((16,)),
            dma((16,)), dma((16,)),
            dma((8,)), dma((32,)),
            dma((16,)), dma,
        ],
        compiler_params=pltpu.CompilerParams(has_side_effects=True),
    )(
        ainv.reshape(1024, 128), second_on_first, lhat_first, lhat_second,
        dinv_first.T, dinv_second.T, anc_first.reshape(1, -1), anc_second.reshape(1, -1),
    )
    return (
        cross1.transpose(0, 2, 1), diag1.T, cross2.transpose(0, 2, 1), link.T, diag2.T,
    )


def solution(mesh):
    return jax.shard_map(
        body,
        mesh=mesh,
        in_specs=(
            P(None, "row", None, "col"),
            P(None, ("row", "col"), None),
            P(None, ("row", "col"), None),
            P(),
            P(None, "col"),
            P(None, "col"),
            P(),
            P(),
        ),
        out_specs=(
            P(None, "row", "col"),
            P(None, "col"),
            P(None, "row", "col"),
            P(None, "col"),
            P(None, "col"),
        ),
        check_vma=False,
    )
```

```python
import functools

import jax
import jax.numpy as jnp
from jax import lax
from jax.experimental import pallas as pl
from jax.experimental.pallas import tpu as pltpu
from jax.sharding import PartitionSpec as P

MESH = pl.DeviceIdType.MESH
F32 = jnp.float32
BF16 = jnp.bfloat16
X, Y, Z = 4, 8, 8
NR, NC = 16, 32


class Phases:
    def __init__(self):
        self.scope = None

    def __call__(self, name):
        if self.scope is not None:
            self.scope.__exit__(None, None, None)
        self.scope = None
        if name:
            self.scope = jax.named_scope(name)
            self.scope.__enter__()


def split(value):
    high = value.astype(BF16)
    return high, (value - high.astype(F32)).astype(BF16)


def mm(left, right):
    return jnp.dot(left, right, preferred_element_type=F32)


def mm3(high, low, both):
    rows, half = high.shape[0], both.shape[1] // 2
    out = mm(jnp.concatenate([high, low], axis=0), both)
    return out[:rows, :half] + (out[rows:, :half] + out[:rows, half:])


def kernel(
    a_hbm, s_hbm, l1_hbm, l2_hbm, d1_hbm, d2_hbm, anc1_hbm, anc2_hbm,
    cross1_ref, diag1_ref, cross2_ref, link_ref, diag2_ref,
    abuf, a_high, a_low, sbuf, s_both, l1_ref, l2_ref, d1_ref, d2_ref, anc1_ref, anc2_ref,
    rbuf, r_both, own, pieces, mbuf, m_both, part_sum, pt, cr,
    ts, tr, ls, lr, r0, tg, tsum, gb, lsum, xt, lk,
    local_sem, a_send, a_recv, my_send, my_recv, mx_send, mx_recv, sc_send, sc_recv,
    qx_send, qx_recv, qy_send, qy_recv, ag_send, ag_recv, dd_send, dd_recv, rs_send, rs_recv, t_send, t_recv, l_send, l_recv,
    tg_send, tg_recv, g_send, g_recv, b_send, b_recv,
):
    phase = Phases()
    phase("p00_greet")
    r, c = lax.axis_index("row"), lax.axis_index("col")
    z, core = r // 2, r % 2
    y, x = c // X, c % X
    right, left, across = (x + 1) % X, (x + X - 1) % X, (x + 2) % X
    base_y = (z + Z - 2 * (y % 4)) % Z
    to_row = 2 * ((2 * (r // 4) + y) % Z) + x // 2
    to_self = jnp.logical_and(to_row == r, y % 4 == r // 4)

    def remote(src, dst, send, recv, row, col):
        return pltpu.make_async_remote_copy(
            src_ref=src, dst_ref=dst, send_sem=send, recv_sem=recv,
            device_id=(row, col), device_id_type=MESH,
        )

    def came(part, recv):
        remote(part, part, l_send, recv, r, c).wait_recv()

    def left_here(part, send):
        remote(part, part, send, l_recv, r, c).wait_send()

    local = [
        pltpu.make_async_copy(src, dst, local_sem.at[i])
        for i, (src, dst) in enumerate(
            [
                (l1_hbm, l1_ref), (l2_hbm, l2_ref), (anc1_hbm, anc1_ref), (anc2_hbm, anc2_ref),
                (s_hbm, sbuf), (a_hbm, abuf.at[x]), (d1_hbm, d1_ref), (d2_hbm, d2_ref),
            ]
        )
    ]
    for copy in local:
        copy.start()

    barrier = pltpu.get_barrier_semaphore()

    def greet(row, col):
        pl.semaphore_signal(barrier, inc=1, device_id=(row, col), device_id_type=MESH)

    for xq in range(4):
        for par in range(2):
            from_row, from_col = (y % 4) * X + xq, 4 * base_y + 2 * core + par

            @pl.when(jnp.logical_not(jnp.logical_and(from_row == r, from_col == c)))
            def _():
                greet(from_row, from_col)

    greet(r, y * X + right)
    greet(r, y * X + left)
    greet(r, y * X + across)
    for d in range(1, Y):
        greet(r, (y + d) % Y * X + x)

    def greet_row(d, carry):
        greet((r + d) % NR, c)
        return carry

    lax.fori_loop(1, NR, greet_row, 0)

    phase("p01_rows")
    nat = lax.broadcasted_iota(jnp.int32, (512, 1), 0)
    target = (nat // 16 % 4) * 128 + (nat // 64) * 16 + nat % 16
    ones = jnp.where(lax.broadcasted_iota(jnp.int32, (512, 512), 1) == target, 1.0, 0.0).astype(BF16)

    def moved(value):
        out = mm(jnp.concatenate(split(value), axis=0), ones)
        return out[:16] + out[16:]

    tile_ids = lax.broadcasted_iota(jnp.int32, (4, 1), 0) * NR + r

    def keeps(anc_ref):
        hits = jnp.where(anc_ref[...] == tile_ids, 1.0, 0.0).astype(F32)
        return jnp.max(hits, axis=1, keepdims=True)

    for copy in local[0:4]:
        copy.wait()
    keep1, keep2 = keeps(anc1_ref), keeps(anc2_ref)
    rows1 = [l1_ref[a] * keep1[a : a + 1] for a in range(4)]
    rows2 = [l2_ref[a] * keep2[a : a + 1] for a in range(4)]
    m1 = jnp.concatenate(rows1, axis=0)
    m1_moved = moved(m1)

    phase("p02_n2")
    local[4].wait()
    sh, sl = split(sbuf[...])
    s_both[:, 0:512] = sh
    s_both[:, 512:1024] = sl
    n2 = jnp.concatenate(rows2, axis=0) - mm3(*split(m1), s_both[...])
    n2_moved = moved(n2)
    for a in range(4):
        yh, s = a % 2, a // 2
        for k in range(4):
            lanes = slice(k * 128, (k + 1) * 128)
            own[yh * 4 + k, s, pl.ds(0, 4, stride=2), :] = m1_moved[a * 4 : a * 4 + 4, lanes]
            own[yh * 4 + k, s, pl.ds(1, 4, stride=2), :] = n2_moved[a * 4 : a * 4 + 4, lanes]
            rbuf[0, a, y, x, pl.ds(k, 4, stride=4), :] = n2[a * 4 : a * 4 + 4, lanes]
            rbuf[1, a, y, x, pl.ds(k, 4, stride=4), :] = rows1[a][:, lanes]

    for copy in local[5:]:
        copy.wait()
    phase("p03_barrier")
    pl.semaphore_wait(barrier, 3 + 7 + 15 + 8 - to_self.astype(jnp.int32))

    phase("p04_send")
    slot = (r % X) * 2 + x % 2
    for yh in range(2):
        for k in range(4):
            to_col = (r // X + 4 * yh) * X + k
            here = jnp.logical_and(to_row == r, c == to_col)
            copy = remote(own.at[yh * 4 + k], pieces.at[slot], sc_send, sc_recv, to_row, to_col)

            @pl.when(jnp.logical_not(here))
            def _():
                copy.start()

            @pl.when(here)
            def _():
                pieces[slot] = own[yh * 4 + k]

    def a_move(at, half, to, recv):
        part = abuf.at[at, pl.ds(half * 512, 512)]
        remote(part, part, a_send, a_recv.at[recv], r, y * X + to).start()

    a_move(x, 0, right, 0)
    a_move(x, 1, left, 1)
    for to in (right, left, across):
        part = rbuf.at[1, 3, y, x]
        remote(part, part, qx_send, qx_recv, r, y * X + to).start()
    a_move(x, 1, right, 2)
    a_move(x, 0, left, 2)

    parts = (4, 3)

    def r_send(w):
        for d in (4, 3, 5, 2, 6, 1, 7):
            part = rbuf.at[w, 0 : parts[w], y, x]
            remote(part, part, my_send.at[w], my_recv.at[w], r, (y + d) % Y * X + x).start()

    def r_part(w, at, half):
        return rbuf.at[w, 0 : parts[w], half * 4 : half * 4 + 4, at]

    def r_move(w, at, half, to, recv):
        part = r_part(w, at, half)
        remote(part, part, mx_send, mx_recv.at[w, recv], r, y * X + to).start()

    def quarter_over_y():
        came(rbuf.at[1, 3, y, 0:3], qx_recv)
        for d in (4, 3, 5, 2, 6, 1, 7):
            part = rbuf.at[1, 3, y]
            remote(part, part, qy_send, qy_recv, r, (y + d) % Y * X + x).start()

    def r_spread(w):
        came(rbuf.at[w, 0 : parts[w], 0:7, x], my_recv.at[w])
        r_move(w, x, 0, right, 0)
        r_move(w, x, 1, left, 1)
        r_move(w, x, 1, right, 2)
        r_move(w, x, 0, left, 2)

    def r_forward(w):
        came(r_part(w, left, 0), mx_recv.at[w, 0])
        r_move(w, left, 0, right, 2)
        came(r_part(w, right, 1), mx_recv.at[w, 1])
        r_move(w, right, 1, left, 2)

    def r_finish(w):
        came(rbuf.at[w, 0 : parts[w], :, 0:2], mx_recv.at[w, 2])
        if w == 1:
            came(rbuf.at[1, 3, 0:7], qy_recv)
        flat = rbuf.at[w].reshape(2048, 128)
        for k in range(4):
            high, low = split(flat[pl.ds(k, 512, stride=4), :])
            r_both[w, k, :, 0:128] = high
            r_both[w, k, :, 128:256] = low

    r_send(0)
    r_send(1)

    phase("p05_scwait")

    @pl.when(to_self)
    def _():
        came(own.at[0:7], sc_recv)

    @pl.when(jnp.logical_not(to_self))
    def _():
        came(own, sc_recv)

    def pair(zs, cs):
        return 2 * ((zs + Z - 2 * (y % 4)) % Z) + cs

    own_pair = pair(z, core)
    for xq in range(4):
        for s in range(2):
            for m in range(2):
                both = [pieces[2 * xq + par, s, pl.ds(m, 4, stride=2), :] for par in range(2)]
                mbuf[m, xq, s, own_pair] = jnp.concatenate(both, axis=0)

    def slab(m, at):
        return mbuf.at[m, :, :, at]

    def to_partner(m, at):
        remote(slab(m, at), slab(m, at), dd_send, dd_recv.at[m], r + 1 - 2 * core, c).start()

    phase("p06_agsend")
    for m in range(2):
        for d in (4, 3, 5, 2, 6, 1, 7):
            to = (z + d) % Z * 2 + core
            part = slab(m, own_pair)
            remote(part, part, ag_send, ag_recv.at[m, z], to, c).start()
        to_partner(m, own_pair)

    phase("p07_await")
    came(abuf.at[left, pl.ds(0, 512)], a_recv.at[0])
    a_move(left, 0, right, 3)
    came(abuf.at[right, pl.ds(512, 512)], a_recv.at[1])
    a_move(right, 1, left, 3)

    phase("p08_n2y")
    r_spread(0)
    quarter_over_y()

    def gathered(m):
        for d in (7, 1, 6, 2, 5, 3, 4):
            zs = (z + d) % Z
            came(slab(m, pair(zs, core)), ag_recv.at[m, zs])
            to_partner(m, pair(zs, core))

    def columns(m):
        came(mbuf.at[m, :, :, 0:8], dd_recv.at[m])
        for xq in range(4):
            for s in range(2):
                high, low = split(mbuf[m, xq, s].reshape(128, 128))
                m_both[m, xq, s * 128 : (s + 1) * 128, 0:128] = high
                m_both[m, xq, s * 128 : (s + 1) * 128, 128:256] = low

    phase("p09_ag0")
    gathered(0)
    phase("p10_dd0")
    columns(0)

    def owner_send(m):
        for d in (4, 3, 5, 2, 6, 1, 7):
            to = (y + d) % Y
            part = pt.at[:, m, pl.ds(pl.multiple_of(to * 16, 16), 16)]
            remote(part, cr.at[m, y], rs_send, rs_recv.at[m], r, to * X + x).start()

    def slot_product(rb, at, m, fresh):
        rows = pl.ds(pl.multiple_of(rb * 128, 128), 128)
        if fresh:
            both = [abuf[at, pl.ds(rb * 256 + s, 128, stride=2), :] for s in range(2)]
            high, low = split(jnp.concatenate(both, axis=1))
            a_high[at, rows] = high
            a_low[at, rows] = low
        else:
            high, low = a_high[at, rows], a_low[at, rows]
        out = mm(high, m_both[m, at])
        return out[:, 0:128] + (out[:, 128:256] + mm(low, m_both[m, at, :, 0:128]))

    def multiply_near(rb, carry):
        total = slot_product(rb, x, 0, True)
        for at in (left, right):
            total = total + slot_product(rb, at, 0, True)
        part_sum[rb] = total
        return carry

    def multiply_across(rb, carry):
        pt[rb, 0] = (part_sum[rb] + slot_product(rb, across, 0, True)).T
        return carry

    def multiply_second(rb, carry):
        total = slot_product(rb, 0, 1, False)
        for at in range(1, X):
            total = total + slot_product(rb, at, 1, False)
        pt[rb, 1] = total.T
        return carry

    phase("p11_anear")
    came(abuf.at[0], a_recv.at[2])
    phase("p12_mmnear")
    lax.fori_loop(0, 4, multiply_near, 0, unroll=True)
    phase("p13_across")
    came(abuf.at[across], a_recv.at[3])
    phase("p13_mm0")
    lax.fori_loop(0, 4, multiply_across, 0, unroll=True)
    owner_send(0)
    phase("p14_ag1")
    gathered(1)
    phase("p14_n2fwd")
    r_forward(0)
    phase("p14_m1y")
    r_spread(1)
    phase("p15_dd1")
    columns(1)
    phase("p16_mm1")
    lax.fori_loop(0, 4, multiply_second, 0, unroll=True)
    owner_send(1)
    r0_full = mm3(*split(d1_ref[...]), s_both[...])
    for k in range(4):
        r0[k] = r0_full[:, k * 128 : (k + 1) * 128]
    phase("p18_n2x")
    r_finish(0)
    def owned(m, keep, out_ref):
        came(cr.at[m, 0:7], rs_recv.at[m])
        mine = pl.ds(pl.multiple_of(y * 16, 16), 16)
        sums = []
        for a in range(4):
            total = pt[a, m, mine]
            for d in range(1, 8):
                total = total + cr[m, (y + d) % Y, a]
            total = -keep[a : a + 1] * total
            out_ref[a] = total
            sums.append(total)
        return split(jnp.concatenate(sums, axis=1))

    def wide(high, low, w, k):
        return mm3(high, low, r_both[w, k])

    phase("p20_c1wait")
    c_high, c_low = owned(0, keep1, cross1_ref)
    phase("p21_link")
    for k in range(4):
        ls[k] = -wide(c_high, c_low, 0, k)

    def link_row(q):
        return NR - 1 - q

    q_own = NR - 1 - r
    collects = q_own < 4

    def send_link(q, carry):
        copy = remote(ls.at[q], lr.at[r], l_send, l_recv, link_row(q), c)

        @pl.when(r != link_row(q))
        def _():
            copy.start()

        return carry

    lax.fori_loop(0, 4, send_link, 0)

    own_tile = z
    holds = core == 1

    def send_sums():
        def send(tile, carry):
            to = 2 * tile + 1
            copy = remote(ts.at[:, tile], tr.at[:, r], t_send, t_recv, to, c)

            @pl.when(to != r)
            def _():
                copy.start()

            return carry

        lax.fori_loop(0, 8, send, 0)

    def send_totals():
        tr[:, r] = ts[:, own_tile]
        came(tr.at[:, 0:15], t_recv)
        total = tr[:, 0]
        for src in range(1, NR):
            total = total + tr[:, src]
        tg[:, own_tile] = total
        tsum[...] = total

        def send(d, carry):
            remote(tsum, tg.at[:, own_tile], tg_send, tg_recv, (r + d) % NR, c).start()
            return carry

        lax.fori_loop(1, NR, send, 0)

    def totals(w):
        return [
            jnp.concatenate([tg[w, 2 * k], tg[w, 2 * k + 1]], axis=0) for k in range(4)
        ]

    phase("p22_m1fwd")
    r_forward(1)
    phase("p24_link")

    @pl.when(collects)
    def _():
        lr[r] = ls[q_own]
        came(lr.at[0:15], l_recv)
        total = lr[0]
        for src in range(1, NR):
            total = total + lr[src]
        lsum[...] = total - r0[q_own]
        for j in range(8):
            to_col = 8 * q_own + j
            copy = remote(lsum, gb.at[c], g_send, g_recv, r, to_col)

            @pl.when(to_col != c)
            def _():
                copy.start()

    phase("p25_c2wait")
    c2_high, c2_low = owned(1, keep2, cross2_ref)
    by_n2 = [wide(c2_high, c2_low, 0, k) for k in range(4)]
    phase("p26_m1x")
    r_finish(1)
    phase("p26_q3")
    high = jnp.concatenate([c_high, c2_high], axis=0)
    low = jnp.concatenate([c_low, c2_low], axis=0)
    by_m1 = [wide(high, low, 1, k) for k in range(4)]
    rest = mm3(*split(jnp.concatenate([part[16:32] for part in by_m1], axis=1)), s_both[...])
    for k in range(4):
        sums = by_n2[k] + rest[:, k * 128 : (k + 1) * 128]
        for half in range(2):
            ts[0, k * 2 + half] = by_m1[k][half * 8 : half * 8 + 8]
            ts[1, k * 2 + half] = sums[half * 8 : half * 8 + 8]

    send_sums()

    root_row = link_row(c // 8)
    is_root = r == root_row

    def link_out():
        gb[c] = lsum[...]
        came(gb.at[0:31], g_recv)
        for k in range(4):
            xt[k] = gb[8 * k : 8 * k + 8].reshape(128, 128).T
        for k in range(4):
            lk[:, k * 128 : (k + 1) * 128] = xt[k, pl.ds(pl.multiple_of(16 * (c % 8), 16), 16), :]

        def send_on(d, carry):
            remote(lk, lk, b_send, b_recv, (r + d) % NR, c).start()
            return carry

        lax.fori_loop(1, NR, send_on, 0)

    phase("p27_twait")

    pl.when(holds)(send_totals)

    phase("p28_root")
    pl.when(is_root)(link_out)
    phase("p29_tgwait")

    @pl.when(holds)
    def _():
        came(tg.at[:, 0:7], tg_recv)

    @pl.when(jnp.logical_not(holds))
    def _():
        came(tg, tg_recv)

    for k, sums in enumerate(totals(0)):
        lanes = slice(k * 128, (k + 1) * 128)
        diag1_ref[:, lanes] = d1_ref[:, lanes] - sums
    sums2 = totals(1)

    phase("p30_lkwait")

    @pl.when(jnp.logical_not(is_root))
    def _():
        came(lk, b_recv)

    phase("p31_tail")
    link = lk[...]
    link_ref[...] = link
    tail = mm3(*split(link), s_both[...])
    for k in range(4):
        lanes = slice(k * 128, (k + 1) * 128)
        diag2_ref[:, lanes] = d2_ref[:, lanes] - (sums2[k] + tail[:, lanes])

    phase("p32_drain")
    left_here(abuf.at[0:3], a_send)
    left_here(rbuf.at[0, :, 0:7, 0], my_send.at[0])
    left_here(rbuf.at[1, 0:3, 0:7, 0], my_send.at[1])
    left_here(rbuf.at[:, 0:3, 0:7], mx_send)
    left_here(rbuf.at[1, 3, 0, 0:3], qx_send)
    left_here(rbuf.at[1, 3, 0:7], qy_send)
    left_here(mbuf.at[:, :, :, 0:7], ag_send)
    left_here(mbuf.at[:, :, :, 0:8], dd_send)
    left_here(cr.at[:, 0:7], rs_send)

    @pl.when(holds)
    def _():
        left_here(tr.at[:, 0:7], t_send)
        left_here(tr.at[:, 0:15], tg_send)

    @pl.when(jnp.logical_not(holds))
    def _():
        left_here(tr.at[:, 0:8], t_send)


    @pl.when(to_self)
    def _():
        left_here(own.at[0:7], sc_send)

    @pl.when(jnp.logical_not(to_self))
    def _():
        left_here(own, sc_send)

    @pl.when(collects)
    def _():
        left_here(lr.at[0:3], l_send)

        @pl.when(is_root)
        def _():
            left_here(gb.at[0:7], g_send)

        @pl.when(jnp.logical_not(is_root))
        def _():
            left_here(gb.at[0:8], g_send)

    @pl.when(jnp.logical_not(collects))
    def _():
        left_here(lr.at[0:4], l_send)

    @pl.when(is_root)
    def _():
        left_here(mbuf.at[0, :, :, 0:15], b_send)

    phase(None)


def hand_out(*refs):
    sems = refs[10]
    copies = [pltpu.make_async_copy(refs[i], refs[5 + i], sems.at[i]) for i in range(5)]
    for copy in copies:
        copy.start()
    for copy in copies:
        copy.wait()


def body(
    ainv, lhat_first, lhat_second, second_on_first, dinv_first, dinv_second, anc_first, anc_second
):
    vmem = pl.BlockSpec(memory_space=pltpu.VMEM)
    hbm = pl.BlockSpec(memory_space=pl.ANY)
    dma = pltpu.SemaphoreType.DMA
    cross = jax.ShapeDtypeStruct((4, 16, 128), F32)
    panel = jax.ShapeDtypeStruct((16, 512), F32)
    found = pl.pallas_call(
        kernel,
        out_shape=tuple(pltpu.VMEM(leaf.shape, F32) for leaf in (cross, panel, cross, panel, panel)),
        in_specs=[hbm] * 8,
        out_specs=(vmem,) * 5,
        scratch_shapes=[
            pltpu.VMEM((4, 1024, 128), F32),
            pltpu.VMEM((4, 512, 256), BF16),
            pltpu.VMEM((4, 512, 256), BF16),
            pltpu.VMEM((512, 512), F32),
            pltpu.VMEM((512, 1024), BF16),
            pltpu.VMEM((4, 4, 512), F32),
            pltpu.VMEM((4, 4, 512), F32),
            pltpu.VMEM((16, 512), F32),
            pltpu.VMEM((16, 512), F32),
            pltpu.VMEM((1, anc_first.shape[0]), jnp.int32),
            pltpu.VMEM((1, anc_second.shape[0]), jnp.int32),
            pltpu.VMEM((2, 4, 8, 4, 16, 128), F32),
            pltpu.VMEM((2, 4, 512, 256), BF16),
            pltpu.VMEM((8, 2, 8, 128), F32),
            pltpu.VMEM((8, 2, 8, 128), F32),
            pltpu.VMEM((2, 4, 2, 16, 8, 128), F32),
            pltpu.VMEM((2, 4, 256, 256), BF16),
            pltpu.VMEM((4, 128, 128), F32),
            pltpu.VMEM((4, 2, 128, 128), F32),
            pltpu.VMEM((2, 8, 4, 16, 128), F32),
            pltpu.VMEM((2, 8, 8, 128), F32),
            pltpu.VMEM((2, 16, 8, 128), F32),
            pltpu.VMEM((4, 16, 128), F32),
            pltpu.VMEM((16, 16, 128), F32),
            pltpu.VMEM((4, 16, 128), F32),
            pltpu.VMEM((2, 8, 8, 128), F32),
            pltpu.VMEM((2, 8, 128), F32),
            pltpu.VMEM((32, 16, 128), F32),
            pltpu.VMEM((16, 128), F32),
            pltpu.VMEM((4, 128, 128), F32),
            pltpu.VMEM((16, 512), F32),
            dma((8,)),
            dma, dma((4,)),
            dma((2,)), dma((2,)),
            dma, dma((2, 3)),
            dma, dma,
            dma, dma,
            dma, dma,
            dma, dma((2, 8)),
            dma, dma((2,)),
            dma, dma((2,)),
            dma, dma,
            dma, dma,
            dma, dma,
            dma, dma,
            dma, dma,
        ],
        compiler_params=pltpu.CompilerParams(collective_id=0, has_side_effects=True),
    )(
        ainv.reshape(1024, 128), second_on_first, lhat_first, lhat_second,
        dinv_first.T, dinv_second.T, anc_first.reshape(1, -1), anc_second.reshape(1, -1),
    )
    cross1, diag1, cross2, link, diag2 = pl.pallas_call(
        hand_out,
        out_shape=(cross, panel, cross, panel, panel),
        in_specs=[vmem] * 5,
        out_specs=(hbm,) * 5,
        scratch_shapes=[dma((5,))],
    )(*[pltpu.with_memory_space_constraint(leaf, pltpu.VMEM) for leaf in found])
    return (
        cross1.transpose(0, 2, 1), diag1.T, cross2.transpose(0, 2, 1), link.T, diag2.T,
    )


def solution(mesh):
    return jax.shard_map(
        body,
        mesh=mesh,
        in_specs=(
            P(None, "row", None, "col"),
            P(None, ("row", "col"), None),
            P(None, ("row", "col"), None),
            P(),
            P(None, "col"),
            P(None, "col"),
            P(),
            P(),
        ),
        out_specs=(
            P(None, "row", "col"),
            P(None, "col"),
            P(None, "row", "col"),
            P(None, "col"),
            P(None, "col"),
        ),
        check_vma=False,
    )
```

```python
import functools

import jax
import jax.numpy as jnp
from jax import lax
from jax.experimental import pallas as pl
from jax.experimental.pallas import tpu as pltpu
from jax.sharding import PartitionSpec as P

MESH = pl.DeviceIdType.MESH
F32 = jnp.float32
BF16 = jnp.bfloat16
X, Y, Z = 4, 8, 8
NR, NC = 16, 32


class Phases:
    def __init__(self):
        self.scope = None

    def __call__(self, name):
        if self.scope is not None:
            self.scope.__exit__(None, None, None)
        self.scope = None
        if name:
            self.scope = jax.named_scope(name)
            self.scope.__enter__()


def split(value):
    high = value.astype(BF16)
    return high, (value - high.astype(F32)).astype(BF16)


def mm(left, right):
    return jnp.dot(left, right, preferred_element_type=F32)


def mm3(high, low, both):
    rows, half = high.shape[0], both.shape[1] // 2
    out = mm(jnp.concatenate([high, low], axis=0), both)
    return out[:rows, :half] + (out[rows:, :half] + out[:rows, half:])


def kernel(
    a_hbm, s_hbm, l1_hbm, l2_hbm, d1_hbm, d2_hbm, anc1_hbm, anc2_hbm,
    cross1_ref, diag1_ref, cross2_ref, link_ref, diag2_ref,
    abuf, a_high, a_low, sbuf, s_both, l1_ref, l2_ref, d1_ref, d2_ref, anc1_ref, anc2_ref,
    rbuf, r_both, own, pieces, mbuf, m_both, part_sum, pt, cr,
    ts, tr, ls, lr, r0, tg, tsum, gb, lsum, xt, lk,
    local_sem, a_send, a_recv, my_send, my_recv, mx_send, mx_recv, sc_send, sc_recv,
    qx_send, qx_recv, qy_send, qy_recv, ag_send, ag_recv, dd_send, dd_recv, rs_send, rs_recv, t_send, t_recv, l_send, l_recv,
    tg_send, tg_recv, g_send, g_recv, b_send, b_recv,
):
    phase = Phases()
    phase("p00_greet")
    r, c = lax.axis_index("row"), lax.axis_index("col")
    z, core = r // 2, r % 2
    y, x = c // X, c % X
    right, left, across = (x + 1) % X, (x + X - 1) % X, (x + 2) % X
    base_y = (z + Z - 2 * (y % 4)) % Z
    to_row = 2 * ((2 * (r // 4) + y) % Z) + x // 2
    to_self = jnp.logical_and(to_row == r, y % 4 == r // 4)

    def remote(src, dst, send, recv, row, col):
        return pltpu.make_async_remote_copy(
            src_ref=src, dst_ref=dst, send_sem=send, recv_sem=recv,
            device_id=(row, col), device_id_type=MESH,
        )

    def came(part, recv):
        remote(part, part, l_send, recv, r, c).wait_recv()

    def left_here(part, send):
        remote(part, part, send, l_recv, r, c).wait_send()

    local = [
        pltpu.make_async_copy(src, dst, local_sem.at[i])
        for i, (src, dst) in enumerate(
            [
                (l1_hbm, l1_ref), (l2_hbm, l2_ref), (anc1_hbm, anc1_ref), (anc2_hbm, anc2_ref),
                (a_hbm, abuf.at[x]), (s_hbm, sbuf), (d1_hbm, d1_ref), (d2_hbm, d2_ref),
            ]
        )
    ]
    for copy in local:
        copy.start()

    barrier = pltpu.get_barrier_semaphore()

    def greet(row, col):
        pl.semaphore_signal(barrier, inc=1, device_id=(row, col), device_id_type=MESH)

    for xq in range(4):
        for par in range(2):
            from_row, from_col = (y % 4) * X + xq, 4 * base_y + 2 * core + par

            @pl.when(jnp.logical_not(jnp.logical_and(from_row == r, from_col == c)))
            def _():
                greet(from_row, from_col)

    greet(r, y * X + right)
    greet(r, y * X + left)
    greet(r, y * X + across)
    for d in range(1, Y):
        greet(r, (y + d) % Y * X + x)

    def greet_row(d, carry):
        greet((r + d) % NR, c)
        return carry

    lax.fori_loop(1, NR, greet_row, 0)

    phase("p01_rows")
    nat = lax.broadcasted_iota(jnp.int32, (512, 1), 0)
    target = (nat // 16 % 4) * 128 + (nat // 64) * 16 + nat % 16
    ones = jnp.where(lax.broadcasted_iota(jnp.int32, (512, 512), 1) == target, 1.0, 0.0).astype(BF16)

    def moved(value):
        out = mm(jnp.concatenate(split(value), axis=0), ones)
        return out[:16] + out[16:]

    tile_ids = lax.broadcasted_iota(jnp.int32, (4, 1), 0) * NR + r

    def keeps(anc_ref):
        hits = jnp.where(anc_ref[...] == tile_ids, 1.0, 0.0).astype(F32)
        return jnp.max(hits, axis=1, keepdims=True)

    for copy in local[0:4]:
        copy.wait()
    keep1, keep2 = keeps(anc1_ref), keeps(anc2_ref)
    rows1 = [l1_ref[a] * keep1[a : a + 1] for a in range(4)]
    rows2 = [l2_ref[a] * keep2[a : a + 1] for a in range(4)]
    m1 = jnp.concatenate(rows1, axis=0)

    def lay_own(m, value):
        for a in range(4):
            for k in range(4):
                part = value[a * 4 : a * 4 + 4, k * 128 : (k + 1) * 128]
                own[m, a % 2 * 4 + k, a // 2 * 4 : a // 2 * 4 + 4] = part

    def lay_rows(w, value):
        for a in range(4):
            for k in range(4):
                part = value[a * 4 : a * 4 + 4, k * 128 : (k + 1) * 128]
                rbuf[w, a, y, x, pl.ds(k, 4, stride=4), :] = part

    lay_own(0, moved(m1))
    lay_rows(1, m1)
    local[4].wait()
    phase("p03_barrier")
    pl.semaphore_wait(barrier, 3 + 7 + 15 + 8 - to_self.astype(jnp.int32))

    phase("p04_send")
    slot = (r % X) * 2 + x % 2

    def scatter(m):
        for yh in range(2):
            for k in range(4):
                to_col = (r // X + 4 * yh) * X + k
                here = jnp.logical_and(to_row == r, c == to_col)
                part = own.at[m, yh * 4 + k]
                copy = remote(part, pieces.at[m, slot], sc_send.at[m], sc_recv.at[m], to_row, to_col)

                @pl.when(jnp.logical_not(here))
                def _():
                    copy.start()

                @pl.when(here)
                def _():
                    pieces[m, slot] = own[m, yh * 4 + k]

    scatter(0)

    def a_move(at, half, to, recv):
        part = abuf.at[at, pl.ds(half * 512, 512)]
        remote(part, part, a_send, a_recv.at[recv], r, y * X + to).start()

    a_move(x, 0, right, 0)
    a_move(x, 1, left, 1)
    for to in (right, left, across):
        part = rbuf.at[1, 3, y, x]
        remote(part, part, qx_send, qx_recv, r, y * X + to).start()
    a_move(x, 1, right, 2)
    a_move(x, 0, left, 2)

    phase("p02_n2")
    for copy in local[5:]:
        copy.wait()
    sh, sl = split(sbuf[...])
    s_both[:, 0:512] = sh
    s_both[:, 512:1024] = sl
    n2 = jnp.concatenate(rows2, axis=0) - mm3(*split(m1), s_both[...])
    lay_own(1, moved(n2))
    lay_rows(0, n2)
    scatter(1)

    parts = (4, 3)

    def r_send(w):
        for d in (4, 3, 5, 2, 6, 1, 7):
            part = rbuf.at[w, 0 : parts[w], y, x]
            remote(part, part, my_send.at[w], my_recv.at[w], r, (y + d) % Y * X + x).start()

    def r_part(w, at, half):
        return rbuf.at[w, 0 : parts[w], half * 4 : half * 4 + 4, at]

    def r_move(w, at, half, to, recv):
        part = r_part(w, at, half)
        remote(part, part, mx_send, mx_recv.at[w, recv], r, y * X + to).start()

    def quarter_over_y():
        came(rbuf.at[1, 3, y, 0:3], qx_recv)
        for d in (4, 3, 5, 2, 6, 1, 7):
            part = rbuf.at[1, 3, y]
            remote(part, part, qy_send, qy_recv, r, (y + d) % Y * X + x).start()

    def r_spread(w):
        came(rbuf.at[w, 0 : parts[w], 0:7, x], my_recv.at[w])
        r_move(w, x, 0, right, 0)
        r_move(w, x, 1, left, 1)
        r_move(w, x, 1, right, 2)
        r_move(w, x, 0, left, 2)

    def r_forward(w):
        came(r_part(w, left, 0), mx_recv.at[w, 0])
        r_move(w, left, 0, right, 2)
        came(r_part(w, right, 1), mx_recv.at[w, 1])
        r_move(w, right, 1, left, 2)

    def r_finish(w):
        came(rbuf.at[w, 0 : parts[w], :, 0:2], mx_recv.at[w, 2])
        if w == 1:
            came(rbuf.at[1, 3, 0:7], qy_recv)
        flat = rbuf.at[w].reshape(2048, 128)
        for k in range(4):
            high, low = split(flat[pl.ds(k, 512, stride=4), :])
            r_both[w, k, :, 0:128] = high
            r_both[w, k, :, 128:256] = low

    r_send(0)
    r_send(1)

    def pair(zs, cs):
        return 2 * ((zs + Z - 2 * (y % 4)) % Z) + cs

    own_pair = pair(z, core)

    def slab(m, at):
        return mbuf.at[m, :, :, at]

    def to_partner(m, at):
        remote(slab(m, at), slab(m, at), dd_send, dd_recv.at[m], r + 1 - 2 * core, c).start()

    def along_z(m):
        @pl.when(to_self)
        def _():
            came(own.at[m, 0:7], sc_recv.at[m])

        @pl.when(jnp.logical_not(to_self))
        def _():
            came(own.at[m], sc_recv.at[m])

        for xq in range(4):
            for s in range(2):
                both = [pieces[m, 2 * xq + par, s * 4 : s * 4 + 4] for par in range(2)]
                mbuf[m, xq, s, own_pair] = jnp.concatenate(both, axis=0)
        for d in (4, 3, 5, 2, 6, 1, 7):
            to = (z + d) % Z * 2 + core
            part = slab(m, own_pair)
            remote(part, part, ag_send, ag_recv.at[m, z], to, c).start()
        to_partner(m, own_pair)

    phase("p05_sc0")
    along_z(0)
    phase("p06_sc1")
    along_z(1)

    phase("p07_await")
    came(abuf.at[left, pl.ds(0, 512)], a_recv.at[0])
    a_move(left, 0, right, 3)
    came(abuf.at[right, pl.ds(512, 512)], a_recv.at[1])
    a_move(right, 1, left, 3)

    phase("p08_n2y")
    r_spread(0)
    quarter_over_y()

    def gathered(m):
        for d in (7, 1, 6, 2, 5, 3, 4):
            zs = (z + d) % Z
            came(slab(m, pair(zs, core)), ag_recv.at[m, zs])
            to_partner(m, pair(zs, core))

    def columns(m):
        came(mbuf.at[m, :, :, 0:8], dd_recv.at[m])
        for xq in range(4):
            for s in range(2):
                high, low = split(mbuf[m, xq, s].reshape(128, 128))
                m_both[m, xq, s * 128 : (s + 1) * 128, 0:128] = high
                m_both[m, xq, s * 128 : (s + 1) * 128, 128:256] = low

    phase("p09_ag0")
    gathered(0)
    phase("p10_dd0")
    columns(0)

    def owner_send(m):
        for d in (4, 3, 5, 2, 6, 1, 7):
            to = (y + d) % Y
            part = pt.at[:, m, pl.ds(pl.multiple_of(to * 16, 16), 16)]
            remote(part, cr.at[m, y], rs_send, rs_recv.at[m], r, to * X + x).start()

    def slot_product(rb, at, m, fresh):
        rows = pl.ds(pl.multiple_of(rb * 128, 128), 128)
        if fresh:
            both = [abuf[at, pl.ds(rb * 256 + s, 128, stride=2), :] for s in range(2)]
            high, low = split(jnp.concatenate(both, axis=1))
            a_high[at, rows] = high
            a_low[at, rows] = low
        else:
            high, low = a_high[at, rows], a_low[at, rows]
        out = mm(high, m_both[m, at])
        return out[:, 0:128] + (out[:, 128:256] + mm(low, m_both[m, at, :, 0:128]))

    def multiply_near(rb, carry):
        total = slot_product(rb, x, 0, True)
        for at in (left, right):
            total = total + slot_product(rb, at, 0, True)
        part_sum[rb] = total
        return carry

    def multiply_across(rb, carry):
        pt[rb, 0] = (part_sum[rb] + slot_product(rb, across, 0, True)).T
        return carry

    def multiply_second(rb, carry):
        total = slot_product(rb, 0, 1, False)
        for at in range(1, X):
            total = total + slot_product(rb, at, 1, False)
        pt[rb, 1] = total.T
        return carry

    phase("p11_anear")
    came(abuf.at[0], a_recv.at[2])
    phase("p12_mmnear")
    lax.fori_loop(0, 4, multiply_near, 0, unroll=True)
    phase("p13_across")
    came(abuf.at[across], a_recv.at[3])
    phase("p13_mm0")
    lax.fori_loop(0, 4, multiply_across, 0, unroll=True)
    owner_send(0)
    phase("p14_ag1")
    gathered(1)
    phase("p14_n2fwd")
    r_forward(0)
    phase("p14_m1y")
    r_spread(1)
    phase("p15_dd1")
    columns(1)
    phase("p16_mm1")
    lax.fori_loop(0, 4, multiply_second, 0, unroll=True)
    owner_send(1)
    r0_full = mm3(*split(d1_ref[...]), s_both[...])
    for k in range(4):
        r0[k] = r0_full[:, k * 128 : (k + 1) * 128]
    phase("p18_n2x")
    r_finish(0)
    def owned(m, keep, out_ref):
        came(cr.at[m, 0:7], rs_recv.at[m])
        mine = pl.ds(pl.multiple_of(y * 16, 16), 16)
        sums = []
        for a in range(4):
            total = pt[a, m, mine]
            for d in range(1, 8):
                total = total + cr[m, (y + d) % Y, a]
            total = -keep[a : a + 1] * total
            out_ref[a] = total
            sums.append(total)
        return split(jnp.concatenate(sums, axis=1))

    def wide(high, low, w, k):
        return mm3(high, low, r_both[w, k])

    phase("p20_c1wait")
    c_high, c_low = owned(0, keep1, cross1_ref)
    phase("p21_link")
    for k in range(4):
        ls[k] = -wide(c_high, c_low, 0, k)

    def link_row(q):
        return NR - 1 - q

    q_own = NR - 1 - r
    collects = q_own < 4

    def send_link(q, carry):
        copy = remote(ls.at[q], lr.at[r], l_send, l_recv, link_row(q), c)

        @pl.when(r != link_row(q))
        def _():
            copy.start()

        return carry

    lax.fori_loop(0, 4, send_link, 0)

    own_tile = z
    holds = core == 1

    def send_sums():
        def send(tile, carry):
            to = 2 * tile + 1
            copy = remote(ts.at[:, tile], tr.at[:, r], t_send, t_recv, to, c)

            @pl.when(to != r)
            def _():
                copy.start()

            return carry

        lax.fori_loop(0, 8, send, 0)

    def send_totals():
        tr[:, r] = ts[:, own_tile]
        came(tr.at[:, 0:15], t_recv)
        total = tr[:, 0]
        for src in range(1, NR):
            total = total + tr[:, src]
        tg[:, own_tile] = total
        tsum[...] = total

        def send(to, carry):
            copy = remote(tsum, tg.at[:, own_tile], tg_send, tg_recv, to, c)

            @pl.when(to != r)
            def _():
                copy.start()

            return carry

        lax.fori_loop(0, NR, send, 0)

    def totals(w):
        return [
            jnp.concatenate([tg[w, 2 * k], tg[w, 2 * k + 1]], axis=0) for k in range(4)
        ]

    phase("p22_m1fwd")
    r_forward(1)
    phase("p24_link")

    @pl.when(collects)
    def _():
        lr[r] = ls[q_own]
        came(lr.at[0:15], l_recv)
        total = lr[0]
        for src in range(1, NR):
            total = total + lr[src]
        lsum[...] = total - r0[q_own]
        for j in range(8):
            to_col = 8 * q_own + j
            copy = remote(lsum, gb.at[c], g_send, g_recv, r, to_col)

            @pl.when(to_col != c)
            def _():
                copy.start()

    phase("p25_c2wait")
    c2_high, c2_low = owned(1, keep2, cross2_ref)
    by_n2 = [wide(c2_high, c2_low, 0, k) for k in range(4)]
    phase("p26_m1x")
    r_finish(1)
    phase("p26_q3")
    high = jnp.concatenate([c_high, c2_high], axis=0)
    low = jnp.concatenate([c_low, c2_low], axis=0)
    by_m1 = [wide(high, low, 1, k) for k in range(4)]
    rest = mm3(*split(jnp.concatenate([part[16:32] for part in by_m1], axis=1)), s_both[...])
    for k in range(4):
        sums = by_n2[k] + rest[:, k * 128 : (k + 1) * 128]
        for half in range(2):
            ts[0, k * 2 + half] = by_m1[k][half * 8 : half * 8 + 8]
            ts[1, k * 2 + half] = sums[half * 8 : half * 8 + 8]

    send_sums()

    root_row = link_row(c // 8)
    is_root = r == root_row

    def link_out():
        gb[c] = lsum[...]
        came(gb.at[0:31], g_recv)
        for k in range(4):
            xt[k] = gb[8 * k : 8 * k + 8].reshape(128, 128).T
        for k in range(4):
            lk[:, k * 128 : (k + 1) * 128] = xt[k, pl.ds(pl.multiple_of(16 * (c % 8), 16), 16), :]

        def send_on(to, carry):
            copy = remote(lk, lk, b_send, b_recv, to, c)

            @pl.when(to != r)
            def _():
                copy.start()

            return carry

        lax.fori_loop(0, NR, send_on, 0)

    phase("p27_twait")

    pl.when(holds)(send_totals)

    phase("p28_root")
    pl.when(is_root)(link_out)
    phase("p29_tgwait")

    @pl.when(holds)
    def _():
        came(tg.at[:, 0:7], tg_recv)

    @pl.when(jnp.logical_not(holds))
    def _():
        came(tg, tg_recv)

    for k, sums in enumerate(totals(0)):
        lanes = slice(k * 128, (k + 1) * 128)
        diag1_ref[:, lanes] = d1_ref[:, lanes] - sums
    sums2 = totals(1)

    phase("p30_lkwait")

    @pl.when(jnp.logical_not(is_root))
    def _():
        came(lk, b_recv)

    phase("p31_tail")
    link = lk[...]
    link_ref[...] = link
    tail = mm3(*split(link), s_both[...])
    for k in range(4):
        lanes = slice(k * 128, (k + 1) * 128)
        diag2_ref[:, lanes] = d2_ref[:, lanes] - (sums2[k] + tail[:, lanes])

    phase("p32_drain")
    left_here(abuf.at[0:3], a_send)
    left_here(rbuf.at[0, :, 0:7, 0], my_send.at[0])
    left_here(rbuf.at[1, 0:3, 0:7, 0], my_send.at[1])
    left_here(rbuf.at[:, 0:3, 0:7], mx_send)
    left_here(rbuf.at[1, 3, 0, 0:3], qx_send)
    left_here(rbuf.at[1, 3, 0:7], qy_send)
    left_here(mbuf.at[:, :, :, 0:7], ag_send)
    left_here(mbuf.at[:, :, :, 0:8], dd_send)
    left_here(cr.at[:, 0:7], rs_send)

    @pl.when(holds)
    def _():
        left_here(tr.at[:, 0:7], t_send)
        left_here(tr.at[:, 0:15], tg_send)

    @pl.when(jnp.logical_not(holds))
    def _():
        left_here(tr.at[:, 0:8], t_send)


    for m in range(2):

        @pl.when(to_self)
        def _():
            left_here(own.at[m, 0:7], sc_send.at[m])

        @pl.when(jnp.logical_not(to_self))
        def _():
            left_here(own.at[m], sc_send.at[m])

    @pl.when(collects)
    def _():
        left_here(lr.at[0:3], l_send)

        @pl.when(is_root)
        def _():
            left_here(gb.at[0:7], g_send)

        @pl.when(jnp.logical_not(is_root))
        def _():
            left_here(gb.at[0:8], g_send)

    @pl.when(jnp.logical_not(collects))
    def _():
        left_here(lr.at[0:4], l_send)

    @pl.when(is_root)
    def _():
        left_here(mbuf.at[0, :, :, 0:15], b_send)

    phase(None)


def hand_out(*refs):
    sems = refs[10]
    copies = [pltpu.make_async_copy(refs[i], refs[5 + i], sems.at[i]) for i in range(5)]
    for copy in copies:
        copy.start()
    for copy in copies:
        copy.wait()


def body(
    ainv, lhat_first, lhat_second, second_on_first, dinv_first, dinv_second, anc_first, anc_second
):
    vmem = pl.BlockSpec(memory_space=pltpu.VMEM)
    hbm = pl.BlockSpec(memory_space=pl.ANY)
    dma = pltpu.SemaphoreType.DMA
    cross = jax.ShapeDtypeStruct((4, 16, 128), F32)
    panel = jax.ShapeDtypeStruct((16, 512), F32)
    found = pl.pallas_call(
        kernel,
        out_shape=tuple(pltpu.VMEM(leaf.shape, F32) for leaf in (cross, panel, cross, panel, panel)),
        in_specs=[hbm] * 8,
        out_specs=(vmem,) * 5,
        scratch_shapes=[
            pltpu.VMEM((4, 1024, 128), F32),
            pltpu.VMEM((4, 512, 256), BF16),
            pltpu.VMEM((4, 512, 256), BF16),
            pltpu.VMEM((512, 512), F32),
            pltpu.VMEM((512, 1024), BF16),
            pltpu.VMEM((4, 4, 512), F32),
            pltpu.VMEM((4, 4, 512), F32),
            pltpu.VMEM((16, 512), F32),
            pltpu.VMEM((16, 512), F32),
            pltpu.VMEM((1, anc_first.shape[0]), jnp.int32),
            pltpu.VMEM((1, anc_second.shape[0]), jnp.int32),
            pltpu.VMEM((2, 4, 8, 4, 16, 128), F32),
            pltpu.VMEM((2, 4, 512, 256), BF16),
            pltpu.VMEM((2, 8, 8, 128), F32),
            pltpu.VMEM((2, 8, 8, 128), F32),
            pltpu.VMEM((2, 4, 2, 16, 8, 128), F32),
            pltpu.VMEM((2, 4, 256, 256), BF16),
            pltpu.VMEM((4, 128, 128), F32),
            pltpu.VMEM((4, 2, 128, 128), F32),
            pltpu.VMEM((2, 8, 4, 16, 128), F32),
            pltpu.VMEM((2, 8, 8, 128), F32),
            pltpu.VMEM((2, 16, 8, 128), F32),
            pltpu.VMEM((4, 16, 128), F32),
            pltpu.VMEM((16, 16, 128), F32),
            pltpu.VMEM((4, 16, 128), F32),
            pltpu.VMEM((2, 8, 8, 128), F32),
            pltpu.VMEM((2, 8, 128), F32),
            pltpu.VMEM((32, 16, 128), F32),
            pltpu.VMEM((16, 128), F32),
            pltpu.VMEM((4, 128, 128), F32),
            pltpu.VMEM((16, 512), F32),
            dma((8,)),
            dma, dma((4,)),
            dma((2,)), dma((2,)),
            dma, dma((2, 3)),
            dma((2,)), dma((2,)),
            dma, dma,
            dma, dma,
            dma, dma((2, 8)),
            dma, dma((2,)),
            dma, dma((2,)),
            dma, dma,
            dma, dma,
            dma, dma,
            dma, dma,
            dma, dma,
        ],
        compiler_params=pltpu.CompilerParams(collective_id=0, has_side_effects=True),
    )(
        ainv.reshape(1024, 128), second_on_first, lhat_first, lhat_second,
        dinv_first.T, dinv_second.T, anc_first.reshape(1, -1), anc_second.reshape(1, -1),
    )
    cross1, diag1, cross2, link, diag2 = pl.pallas_call(
        hand_out,
        out_shape=(cross, panel, cross, panel, panel),
        in_specs=[vmem] * 5,
        out_specs=(hbm,) * 5,
        scratch_shapes=[dma((5,))],
    )(*[pltpu.with_memory_space_constraint(leaf, pltpu.VMEM) for leaf in found])
    return (
        cross1.transpose(0, 2, 1), diag1.T, cross2.transpose(0, 2, 1), link.T, diag2.T,
    )


def solution(mesh):
    return jax.shard_map(
        body,
        mesh=mesh,
        in_specs=(
            P(None, "row", None, "col"),
            P(None, ("row", "col"), None),
            P(None, ("row", "col"), None),
            P(),
            P(None, "col"),
            P(None, "col"),
            P(),
            P(),
        ),
        out_specs=(
            P(None, "row", "col"),
            P(None, "col"),
            P(None, "row", "col"),
            P(None, "col"),
            P(None, "col"),
        ),
        check_vma=False,
    )
```

```python
import functools

import jax
import jax.numpy as jnp
from jax import lax
from jax.experimental import pallas as pl
from jax.experimental.pallas import tpu as pltpu
from jax.sharding import PartitionSpec as P

MESH = pl.DeviceIdType.MESH
F32 = jnp.float32
BF16 = jnp.bfloat16
X, Y, Z = 4, 8, 8
NR, NC = 16, 32


class Phases:
    def __init__(self):
        self.scope = None

    def __call__(self, name):
        if self.scope is not None:
            self.scope.__exit__(None, None, None)
        self.scope = None
        if name:
            self.scope = jax.named_scope(name)
            self.scope.__enter__()


def split(value):
    high = value.astype(BF16)
    return high, (value - high.astype(F32)).astype(BF16)


def mm(left, right):
    return jnp.dot(left, right, preferred_element_type=F32)


def mm3(high, low, both):
    rows, half = high.shape[0], both.shape[1] // 2
    out = mm(jnp.concatenate([high, low], axis=0), both)
    return out[:rows, :half] + (out[rows:, :half] + out[:rows, half:])


def kernel(
    a_hbm, s_hbm, l1_hbm, l2_hbm, d1_hbm, d2_hbm, anc1_hbm, anc2_hbm,
    cross1_ref, diag1_ref, cross2_ref, link_ref, diag2_ref,
    abuf, a_high, a_low, sbuf, s_both, l1_ref, l2_ref, d1_ref, d2_ref, anc1_ref, anc2_ref,
    rbuf, r_both, own, pieces, mbuf, m_both, part_sum, pt, cr,
    ts, tr, ls, lr, r0, tg, tsum, gb, lsum, xt, lk,
    local_sem, a_send, a_recv, my_send, my_recv, mx_send, mx_recv, sc_send, sc_recv,
    qx_send, qx_recv, qy_send, qy_recv, ag_send, ag_recv, dd_send, dd_recv, rs_send, rs_recv, t_send, t_recv, l_send, l_recv,
    tg_send, tg_recv, g_send, g_recv, b_send, b_recv,
):
    phase = Phases()
    phase("p00_greet")
    r, c = lax.axis_index("row"), lax.axis_index("col")
    z, core = r // 2, r % 2
    y, x = c // X, c % X
    right, left, across = (x + 1) % X, (x + X - 1) % X, (x + 2) % X
    base_y = (z + Z - 2 * (y % 4)) % Z
    to_row = 2 * ((2 * (r // 4) + y) % Z) + x // 2
    to_self = jnp.logical_and(to_row == r, y % 4 == r // 4)

    def remote(src, dst, send, recv, row, col):
        return pltpu.make_async_remote_copy(
            src_ref=src, dst_ref=dst, send_sem=send, recv_sem=recv,
            device_id=(row, col), device_id_type=MESH,
        )

    def came(part, recv):
        remote(part, part, l_send, recv, r, c).wait_recv()

    def left_here(part, send):
        remote(part, part, send, l_recv, r, c).wait_send()

    local = [
        pltpu.make_async_copy(src, dst, local_sem.at[i])
        for i, (src, dst) in enumerate(
            [
                (l1_hbm, l1_ref), (l2_hbm, l2_ref), (anc1_hbm, anc1_ref), (anc2_hbm, anc2_ref),
                (a_hbm, abuf.at[x]), (s_hbm, sbuf), (d1_hbm, d1_ref), (d2_hbm, d2_ref),
            ]
        )
    ]
    for copy in local:
        copy.start()

    barrier = pltpu.get_barrier_semaphore()

    def greet(row, col):
        pl.semaphore_signal(barrier, inc=1, device_id=(row, col), device_id_type=MESH)

    for xq in range(4):
        for par in range(2):
            from_row, from_col = (y % 4) * X + xq, 4 * base_y + 2 * core + par

            @pl.when(jnp.logical_not(jnp.logical_and(from_row == r, from_col == c)))
            def _():
                greet(from_row, from_col)

    greet(r, y * X + right)
    greet(r, y * X + left)
    greet(r, y * X + across)
    for d in range(1, Y):
        greet(r, (y + d) % Y * X + x)

    def greet_row(d, carry):
        greet((r + d) % NR, c)
        return carry

    lax.fori_loop(1, NR, greet_row, 0)

    phase("p01_rows")
    nat = lax.broadcasted_iota(jnp.int32, (512, 1), 0)
    target = (nat // 16 % 4) * 128 + (nat // 64) * 16 + nat % 16
    ones = jnp.where(lax.broadcasted_iota(jnp.int32, (512, 512), 1) == target, 1.0, 0.0).astype(BF16)

    def moved(value):
        out = mm(jnp.concatenate(split(value), axis=0), ones)
        return out[:16] + out[16:]

    tile_ids = lax.broadcasted_iota(jnp.int32, (4, 1), 0) * NR + r

    def keeps(anc_ref):
        hits = jnp.where(anc_ref[...] == tile_ids, 1.0, 0.0).astype(F32)
        return jnp.max(hits, axis=1, keepdims=True)

    for copy in local[0:4]:
        copy.wait()
    keep1, keep2 = keeps(anc1_ref), keeps(anc2_ref)
    rows1 = [l1_ref[a] * keep1[a : a + 1] for a in range(4)]
    rows2 = [l2_ref[a] * keep2[a : a + 1] for a in range(4)]
    m1 = jnp.concatenate(rows1, axis=0)

    def lay_own(m, value):
        for a in range(4):
            for k in range(4):
                part = value[a * 4 : a * 4 + 4, k * 128 : (k + 1) * 128]
                own[m, a % 2 * 4 + k, a // 2 * 4 : a // 2 * 4 + 4] = part

    def lay_rows(w, value):
        for a in range(4):
            for k in range(4):
                part = value[a * 4 : a * 4 + 4, k * 128 : (k + 1) * 128]
                rbuf[w, a, y, x, pl.ds(k, 4, stride=4), :] = part

    lay_own(0, moved(m1))
    lay_rows(1, m1)
    local[4].wait()
    phase("p03_barrier")
    pl.semaphore_wait(barrier, 3 + 7 + 15 + 8 - to_self.astype(jnp.int32))

    phase("p04_send")
    slot = (r % X) * 2 + x % 2

    def scatter(m):
        for yh in range(2):
            for k in range(4):
                to_col = (r // X + 4 * yh) * X + k
                here = jnp.logical_and(to_row == r, c == to_col)
                part = own.at[m, yh * 4 + k]
                copy = remote(part, pieces.at[m, slot], sc_send.at[m], sc_recv.at[m], to_row, to_col)

                @pl.when(jnp.logical_not(here))
                def _():
                    copy.start()

                @pl.when(here)
                def _():
                    pieces[m, slot] = own[m, yh * 4 + k]

    scatter(0)

    def a_move(at, half, to, recv):
        part = abuf.at[at, pl.ds(half * 512, 512)]
        remote(part, part, a_send, a_recv.at[recv], r, y * X + to).start()

    a_move(x, 0, right, 0)
    a_move(x, 1, left, 1)
    for to in (right, left, across):
        part = rbuf.at[1, 3, y, x]
        remote(part, part, qx_send, qx_recv, r, y * X + to).start()
    a_move(x, 1, right, 2)
    a_move(x, 0, left, 2)

    phase("p02_n2")
    for copy in local[5:]:
        copy.wait()
    sh, sl = split(sbuf[...])
    s_both[:, 0:512] = sh
    s_both[:, 512:1024] = sl
    n2 = jnp.concatenate(rows2, axis=0) - mm3(*split(m1), s_both[...])
    lay_own(1, moved(n2))
    lay_rows(0, n2)
    scatter(1)

    parts = (4, 3)

    def r_send(w):
        for d in (4, 3, 5, 2, 6, 1, 7):
            part = rbuf.at[w, 0 : parts[w], y, x]
            remote(part, part, my_send.at[w], my_recv.at[w], r, (y + d) % Y * X + x).start()

    def r_part(w, at, half):
        return rbuf.at[w, 0 : parts[w], half * 4 : half * 4 + 4, at]

    def r_move(w, at, half, to, recv):
        part = r_part(w, at, half)
        remote(part, part, mx_send, mx_recv.at[w, recv], r, y * X + to).start()

    def quarter_over_y():
        came(rbuf.at[1, 3, y, 0:3], qx_recv)
        for d in (4, 3, 5, 2, 6, 1, 7):
            part = rbuf.at[1, 3, y]
            remote(part, part, qy_send, qy_recv, r, (y + d) % Y * X + x).start()

    def r_spread(w):
        came(rbuf.at[w, 0 : parts[w], 0:7, x], my_recv.at[w])
        r_move(w, x, 0, right, 0)
        r_move(w, x, 1, left, 1)
        r_move(w, x, 1, right, 2)
        r_move(w, x, 0, left, 2)

    def r_forward(w):
        came(r_part(w, left, 0), mx_recv.at[w, 0])
        r_move(w, left, 0, right, 2)
        came(r_part(w, right, 1), mx_recv.at[w, 1])
        r_move(w, right, 1, left, 2)

    def r_finish(w):
        came(rbuf.at[w, 0 : parts[w], :, 0:2], mx_recv.at[w, 2])
        if w == 1:
            came(rbuf.at[1, 3, 0:7], qy_recv)
        flat = rbuf.at[w].reshape(2048, 128)
        for k in range(4):
            high, low = split(flat[pl.ds(k, 512, stride=4), :])
            r_both[w, k, :, 0:128] = high
            r_both[w, k, :, 128:256] = low

    r_send(0)
    r_send(1)

    def pair(zs, cs):
        return 2 * ((zs + Z - 2 * (y % 4)) % Z) + cs

    own_pair = pair(z, core)

    def slab(m, at):
        return mbuf.at[m, :, :, at]

    def to_partner(m, at):
        remote(slab(m, at), slab(m, at), dd_send, dd_recv.at[m], r + 1 - 2 * core, c).start()

    def along_z(m):
        @pl.when(to_self)
        def _():
            came(own.at[m, 0:7], sc_recv.at[m])

        @pl.when(jnp.logical_not(to_self))
        def _():
            came(own.at[m], sc_recv.at[m])

        for xq in range(4):
            for s in range(2):
                both = [pieces[m, 2 * xq + par, s * 4 : s * 4 + 4] for par in range(2)]
                mbuf[m, xq, s, own_pair] = jnp.concatenate(both, axis=0)
        for d in (4, 3, 5, 2, 6, 1, 7):
            to = (z + d) % Z * 2 + core
            part = slab(m, own_pair)
            remote(part, part, ag_send, ag_recv.at[m, z], to, c).start()
        to_partner(m, own_pair)

    phase("p05_sc0")
    along_z(0)
    phase("p06_sc1")
    along_z(1)

    phase("p07_await")
    came(abuf.at[left, pl.ds(0, 512)], a_recv.at[0])
    a_move(left, 0, right, 3)
    came(abuf.at[right, pl.ds(512, 512)], a_recv.at[1])
    a_move(right, 1, left, 3)

    phase("p08_n2y")
    r_spread(0)
    quarter_over_y()

    def gathered(m):
        for d in (7, 1, 6, 2, 5, 3, 4):
            zs = (z + d) % Z
            came(slab(m, pair(zs, core)), ag_recv.at[m, zs])
            to_partner(m, pair(zs, core))

    def columns(m):
        came(mbuf.at[m, :, :, 0:8], dd_recv.at[m])
        for xq in range(4):
            for s in range(2):
                high, low = split(mbuf[m, xq, s].reshape(128, 128))
                m_both[m, xq, s * 128 : (s + 1) * 128, 0:128] = high
                m_both[m, xq, s * 128 : (s + 1) * 128, 128:256] = low

    phase("p09_ag0")
    gathered(0)
    phase("p10_dd0")
    columns(0)

    def owner_send(m):
        for d in (4, 3, 5, 2, 6, 1, 7):
            to = (y + d) % Y
            part = pt.at[:, m, pl.ds(pl.multiple_of(to * 16, 16), 16)]
            remote(part, cr.at[m, y], rs_send, rs_recv.at[m], r, to * X + x).start()

    def slot_product(rb, at, m, fresh):
        rows = pl.ds(pl.multiple_of(rb * 128, 128), 128)
        if fresh:
            both = [abuf[at, pl.ds(rb * 256 + s, 128, stride=2), :] for s in range(2)]
            high, low = split(jnp.concatenate(both, axis=1))
            a_high[at, rows] = high
            a_low[at, rows] = low
        else:
            high, low = a_high[at, rows], a_low[at, rows]
        out = mm(high, m_both[m, at])
        return out[:, 0:128] + (out[:, 128:256] + mm(low, m_both[m, at, :, 0:128]))

    def multiply_near(rb, carry):
        total = slot_product(rb, x, 0, True)
        for at in (left, right):
            total = total + slot_product(rb, at, 0, True)
        part_sum[rb] = total
        return carry

    def multiply_across(rb, carry):
        pt[rb, 0] = (part_sum[rb] + slot_product(rb, across, 0, True)).T
        return carry

    def multiply_second(rb, carry):
        total = slot_product(rb, 0, 1, False)
        for at in range(1, X):
            total = total + slot_product(rb, at, 1, False)
        pt[rb, 1] = total.T
        return carry

    phase("p11_anear")
    came(abuf.at[0], a_recv.at[2])
    phase("p12_mmnear")
    lax.fori_loop(0, 4, multiply_near, 0, unroll=True)
    phase("p13_across")
    came(abuf.at[across], a_recv.at[3])
    phase("p13_mm0")
    lax.fori_loop(0, 4, multiply_across, 0, unroll=True)
    owner_send(0)
    phase("p14_ag1")
    gathered(1)
    phase("p14_n2fwd")
    r_forward(0)
    phase("p14_m1y")
    r_spread(1)
    phase("p15_dd1")
    columns(1)
    phase("p16_mm1")
    lax.fori_loop(0, 4, multiply_second, 0, unroll=True)
    owner_send(1)
    r0_full = mm3(*split(d1_ref[...]), s_both[...])
    for k in range(4):
        r0[k] = r0_full[:, k * 128 : (k + 1) * 128]
    phase("p18_n2x")
    r_finish(0)
    def owned(m, keep, out_ref):
        came(cr.at[m, 0:7], rs_recv.at[m])
        mine = pl.ds(pl.multiple_of(y * 16, 16), 16)
        sums = []
        for a in range(4):
            total = pt[a, m, mine]
            for d in range(1, 8):
                total = total + cr[m, (y + d) % Y, a]
            total = -keep[a : a + 1] * total
            out_ref[a] = total
            sums.append(total)
        return split(jnp.concatenate(sums, axis=1))

    def wide(high, low, w, k):
        return mm3(high, low, r_both[w, k])

    phase("p20_c1wait")
    c_high, c_low = owned(0, keep1, cross1_ref)
    phase("p21_link")
    for k in range(4):
        ls[k] = -wide(c_high, c_low, 0, k)

    def link_row(q):
        return NR - 1 - 2 * q

    q_own = (NR - 1 - r) // 2
    collects = jnp.logical_and(core == 1, q_own < 4)

    def send_link(q, carry):
        copy = remote(ls.at[q], lr.at[r], l_send, l_recv, link_row(q), c)

        @pl.when(r != link_row(q))
        def _():
            copy.start()

        return carry

    lax.fori_loop(0, 4, send_link, 0)

    own_tile = z
    holds = core == 1 - z // 4

    def send_sums():
        def send(tile, carry):
            to = 2 * tile + 1 - tile // 4
            copy = remote(ts.at[:, tile], tr.at[:, r], t_send, t_recv, to, c)

            @pl.when(to != r)
            def _():
                copy.start()

            return carry

        lax.fori_loop(0, 8, send, 0)

    def send_totals():
        tr[:, r] = ts[:, own_tile]
        came(tr.at[:, 0:15], t_recv)
        total = tr[:, 0]
        for src in range(1, NR):
            total = total + tr[:, src]
        tg[:, own_tile] = total
        tsum[...] = total

        def send(to, carry):
            copy = remote(tsum, tg.at[:, own_tile], tg_send, tg_recv, to, c)

            @pl.when(to != r)
            def _():
                copy.start()

            return carry

        lax.fori_loop(0, NR, send, 0)

    def totals(w):
        return [
            jnp.concatenate([tg[w, 2 * k], tg[w, 2 * k + 1]], axis=0) for k in range(4)
        ]

    phase("p22_m1fwd")
    r_forward(1)
    phase("p24_link")

    @pl.when(collects)
    def _():
        lr[r] = ls[q_own]
        came(lr.at[0:15], l_recv)
        total = lr[0]
        for src in range(1, NR):
            total = total + lr[src]
        lsum[...] = total - r0[q_own]
        for j in range(8):
            to_col = 8 * q_own + j
            copy = remote(lsum, gb.at[c], g_send, g_recv, r, to_col)

            @pl.when(to_col != c)
            def _():
                copy.start()

    phase("p25_c2wait")
    c2_high, c2_low = owned(1, keep2, cross2_ref)
    by_n2 = [wide(c2_high, c2_low, 0, k) for k in range(4)]
    phase("p26_m1x")
    r_finish(1)
    phase("p26_q3")
    high = jnp.concatenate([c_high, c2_high], axis=0)
    low = jnp.concatenate([c_low, c2_low], axis=0)
    by_m1 = [wide(high, low, 1, k) for k in range(4)]
    rest = mm3(*split(jnp.concatenate([part[16:32] for part in by_m1], axis=1)), s_both[...])
    for k in range(4):
        sums = by_n2[k] + rest[:, k * 128 : (k + 1) * 128]
        for half in range(2):
            ts[0, k * 2 + half] = by_m1[k][half * 8 : half * 8 + 8]
            ts[1, k * 2 + half] = sums[half * 8 : half * 8 + 8]

    send_sums()

    root_row = link_row(c // 8)
    is_root = r == root_row

    def link_out():
        gb[c] = lsum[...]
        came(gb.at[0:31], g_recv)
        for k in range(4):
            xt[k] = gb[8 * k : 8 * k + 8].reshape(128, 128).T
        for k in range(4):
            lk[:, k * 128 : (k + 1) * 128] = xt[k, pl.ds(pl.multiple_of(16 * (c % 8), 16), 16), :]

        def send_on(to, carry):
            copy = remote(lk, lk, b_send, b_recv, to, c)

            @pl.when(to != r)
            def _():
                copy.start()

            return carry

        lax.fori_loop(0, NR, send_on, 0)

    phase("p27_twait")

    pl.when(holds)(send_totals)

    phase("p28_root")
    pl.when(is_root)(link_out)
    phase("p29_tgwait")

    @pl.when(holds)
    def _():
        came(tg.at[:, 0:7], tg_recv)

    @pl.when(jnp.logical_not(holds))
    def _():
        came(tg, tg_recv)

    for k, sums in enumerate(totals(0)):
        lanes = slice(k * 128, (k + 1) * 128)
        diag1_ref[:, lanes] = d1_ref[:, lanes] - sums
    sums2 = totals(1)

    phase("p30_lkwait")

    @pl.when(jnp.logical_not(is_root))
    def _():
        came(lk, b_recv)

    phase("p31_tail")
    link = lk[...]
    link_ref[...] = link
    tail = mm3(*split(link), s_both[...])
    for k in range(4):
        lanes = slice(k * 128, (k + 1) * 128)
        diag2_ref[:, lanes] = d2_ref[:, lanes] - (sums2[k] + tail[:, lanes])

    phase("p32_drain")
    left_here(abuf.at[0:3], a_send)
    left_here(rbuf.at[0, :, 0:7, 0], my_send.at[0])
    left_here(rbuf.at[1, 0:3, 0:7, 0], my_send.at[1])
    left_here(rbuf.at[:, 0:3, 0:7], mx_send)
    left_here(rbuf.at[1, 3, 0, 0:3], qx_send)
    left_here(rbuf.at[1, 3, 0:7], qy_send)
    left_here(mbuf.at[:, :, :, 0:7], ag_send)
    left_here(mbuf.at[:, :, :, 0:8], dd_send)
    left_here(cr.at[:, 0:7], rs_send)

    @pl.when(holds)
    def _():
        left_here(tr.at[:, 0:7], t_send)
        left_here(tr.at[:, 0:15], tg_send)

    @pl.when(jnp.logical_not(holds))
    def _():
        left_here(tr.at[:, 0:8], t_send)


    for m in range(2):

        @pl.when(to_self)
        def _():
            left_here(own.at[m, 0:7], sc_send.at[m])

        @pl.when(jnp.logical_not(to_self))
        def _():
            left_here(own.at[m], sc_send.at[m])

    @pl.when(collects)
    def _():
        left_here(lr.at[0:3], l_send)

        @pl.when(is_root)
        def _():
            left_here(gb.at[0:7], g_send)

        @pl.when(jnp.logical_not(is_root))
        def _():
            left_here(gb.at[0:8], g_send)

    @pl.when(jnp.logical_not(collects))
    def _():
        left_here(lr.at[0:4], l_send)

    @pl.when(is_root)
    def _():
        left_here(mbuf.at[0, :, :, 0:15], b_send)

    phase(None)


def hand_out(*refs):
    sems = refs[10]
    copies = [pltpu.make_async_copy(refs[i], refs[5 + i], sems.at[i]) for i in range(5)]
    for copy in copies:
        copy.start()
    for copy in copies:
        copy.wait()


def body(
    ainv, lhat_first, lhat_second, second_on_first, dinv_first, dinv_second, anc_first, anc_second
):
    vmem = pl.BlockSpec(memory_space=pltpu.VMEM)
    hbm = pl.BlockSpec(memory_space=pl.ANY)
    dma = pltpu.SemaphoreType.DMA
    cross = jax.ShapeDtypeStruct((4, 16, 128), F32)
    panel = jax.ShapeDtypeStruct((16, 512), F32)
    found = pl.pallas_call(
        kernel,
        out_shape=tuple(pltpu.VMEM(leaf.shape, F32) for leaf in (cross, panel, cross, panel, panel)),
        in_specs=[hbm] * 8,
        out_specs=(vmem,) * 5,
        scratch_shapes=[
            pltpu.VMEM((4, 1024, 128), F32),
            pltpu.VMEM((4, 512, 256), BF16),
            pltpu.VMEM((4, 512, 256), BF16),
            pltpu.VMEM((512, 512), F32),
            pltpu.VMEM((512, 1024), BF16),
            pltpu.VMEM((4, 4, 512), F32),
            pltpu.VMEM((4, 4, 512), F32),
            pltpu.VMEM((16, 512), F32),
            pltpu.VMEM((16, 512), F32),
            pltpu.VMEM((1, anc_first.shape[0]), jnp.int32),
            pltpu.VMEM((1, anc_second.shape[0]), jnp.int32),
            pltpu.VMEM((2, 4, 8, 4, 16, 128), F32),
            pltpu.VMEM((2, 4, 512, 256), BF16),
            pltpu.VMEM((2, 8, 8, 128), F32),
            pltpu.VMEM((2, 8, 8, 128), F32),
            pltpu.VMEM((2, 4, 2, 16, 8, 128), F32),
            pltpu.VMEM((2, 4, 256, 256), BF16),
            pltpu.VMEM((4, 128, 128), F32),
            pltpu.VMEM((4, 2, 128, 128), F32),
            pltpu.VMEM((2, 8, 4, 16, 128), F32),
            pltpu.VMEM((2, 8, 8, 128), F32),
            pltpu.VMEM((2, 16, 8, 128), F32),
            pltpu.VMEM((4, 16, 128), F32),
            pltpu.VMEM((16, 16, 128), F32),
            pltpu.VMEM((4, 16, 128), F32),
            pltpu.VMEM((2, 8, 8, 128), F32),
            pltpu.VMEM((2, 8, 128), F32),
            pltpu.VMEM((32, 16, 128), F32),
            pltpu.VMEM((16, 128), F32),
            pltpu.VMEM((4, 128, 128), F32),
            pltpu.VMEM((16, 512), F32),
            dma((8,)),
            dma, dma((4,)),
            dma((2,)), dma((2,)),
            dma, dma((2, 3)),
            dma((2,)), dma((2,)),
            dma, dma,
            dma, dma,
            dma, dma((2, 8)),
            dma, dma((2,)),
            dma, dma((2,)),
            dma, dma,
            dma, dma,
            dma, dma,
            dma, dma,
            dma, dma,
        ],
        compiler_params=pltpu.CompilerParams(collective_id=0, has_side_effects=True),
    )(
        ainv.reshape(1024, 128), second_on_first, lhat_first, lhat_second,
        dinv_first.T, dinv_second.T, anc_first.reshape(1, -1), anc_second.reshape(1, -1),
    )
    cross1, diag1, cross2, link, diag2 = pl.pallas_call(
        hand_out,
        out_shape=(cross, panel, cross, panel, panel),
        in_specs=[vmem] * 5,
        out_specs=(hbm,) * 5,
        scratch_shapes=[dma((5,))],
    )(*[pltpu.with_memory_space_constraint(leaf, pltpu.VMEM) for leaf in found])
    return (
        cross1.transpose(0, 2, 1), diag1.T, cross2.transpose(0, 2, 1), link.T, diag2.T,
    )


def solution(mesh):
    return jax.shard_map(
        body,
        mesh=mesh,
        in_specs=(
            P(None, "row", None, "col"),
            P(None, ("row", "col"), None),
            P(None, ("row", "col"), None),
            P(),
            P(None, "col"),
            P(None, "col"),
            P(),
            P(),
        ),
        out_specs=(
            P(None, "row", "col"),
            P(None, "col"),
            P(None, "row", "col"),
            P(None, "col"),
            P(None, "col"),
        ),
        check_vma=False,
    )
```
